32 devices in a mesh: dp: 4 (over y, z), tp: 8 (over x, core).
Axes of the slice: x: 4, y: 2, z: 2, core: 2. Of those that a mesh axis runs over, the one named last changes fastest.
The devices are a block of a 4x4x8 slice.
Arguments:
- token_act: bfloat16 [64, 512, 768], P('dp'), parts along dimension 0
- token_cond: bfloat16 [64, 512, 384], P('dp'), parts along dimension 0
- pair_bias: bfloat16 [2, 16, 512, 512], P(None, 'tp')
- token_mask: int32 [512], replicated
- ada_scale: float32 [2, 2, 384], replicated
- ada_w: bfloat16 [2, 2, 384, 2, 768], replicated
- ada_bias: float32 [2, 2, 768], replicated
- zero_w: bfloat16 [2, 384, 2, 768], replicated
- zero_b: float32 [2, 2, 768], replicated
- w_qkvg: bfloat16 [2, 768, 4, 768], P(None, None, None, 'tp')
- b_q: float32 [2, 768], P(None, 'tp')
- w_o: bfloat16 [2, 768, 768], P(None, 'tp')
- w_up: bfloat16 [2, 768, 2, 1536], P(None, None, None, 'tp')
- w_down: bfloat16 [2, 1536, 768], P(None, 'tp')
Outputs:
- output: bfloat16 [64, 512, 768], P('dp'), parts along dimension 0
There are 4 independent parts. The reference program is written for one: setup_inputs(seed, part) draws one part's arguments, and reference() takes and returns one part's arrays. A program takes and returns all parts, laid end to end along the dimension named above; an argument that names none is the same for every part.
All inputs are finite; a program needn't handle non-finite values.
Results may differ from the reference program's by a relative error of at most 0.0181938.
Values are sent between devices in bfloat16 or wider.
A program may use at most 768 MiB of HBM per device.

```python
import math
import jax
import jax.numpy as jnp
from jax import lax

SAMPLES = 16
TOKENS = 512
TOKEN_DIM = 768
COND_DIM = 384
NUM_HEADS = 16
HEAD_DIM = 48
HIDDEN_DIM = 1536
BLOCKS = 2

LN_EPS = 1e-5
BIAS_SCALE = math.sqrt(math.log(TOKENS / 4.0))


def layer_norm(values_in):
    row_mean = jnp.mean(values_in, axis=-1, keepdims=True)
    centered = values_in - row_mean
    variance = jnp.mean(centered * centered, axis=-1, keepdims=True)
    return centered * lax.rsqrt(variance + LN_EPS)


def ada_norm(act_f32, cond_normed, scale_vec, weight, bias_vec):
    cond_in = (cond_normed * scale_vec).astype(jnp.bfloat16)
    modulation = jnp.dot(cond_in, weight.reshape(COND_DIM, 2 * TOKEN_DIM), preferred_element_type=jnp.float32)
    modulation = modulation.reshape(-1, 2, TOKEN_DIM)
    return (jax.nn.sigmoid(modulation[:, 0] + bias_vec) * layer_norm(act_f32) + modulation[:, 1]).astype(jnp.bfloat16)


def setup_inputs(seed: int = 0, part: int = 0) -> dict:
    root_key = jax.random.key(seed)
    shared_keys = jax.random.split(root_key, 12)
    part_keys = jax.random.split(jax.random.fold_in(shared_keys[11], part), 2)
    token_act = jax.random.normal(part_keys[0], (SAMPLES, TOKENS, TOKEN_DIM), jnp.float32)
    token_cond = jax.random.normal(part_keys[1], (SAMPLES, TOKENS, COND_DIM), jnp.float32)
    pair_bias = BIAS_SCALE * jax.random.normal(shared_keys[0], (BLOCKS, NUM_HEADS, TOKENS, TOKENS), jnp.float32)
    keep_draw = jax.random.randint(shared_keys[1], (TOKENS,), 0, 4)
    token_mask = jnp.where((keep_draw != 0) | (jnp.arange(TOKENS) == 0), 1, 0).astype(jnp.int32)
    cond_gain = COND_DIM ** -0.5
    width_gain = TOKEN_DIM ** -0.5
    hidden_gain = HIDDEN_DIM ** -0.5
    ada_scale = 1.0 + 0.5 * jax.random.normal(shared_keys[2], (BLOCKS, 2, COND_DIM), jnp.float32)
    ada_w = cond_gain * jax.random.normal(shared_keys[3], (BLOCKS, 2, COND_DIM, 2, TOKEN_DIM), jnp.float32)
    ada_bias = jax.random.normal(shared_keys[4], (BLOCKS, 2, TOKEN_DIM), jnp.float32)
    zero_w = cond_gain * jax.random.normal(shared_keys[5], (BLOCKS, COND_DIM, 2, TOKEN_DIM), jnp.float32)
    zero_b = jax.random.normal(shared_keys[6], (BLOCKS, 2, TOKEN_DIM), jnp.float32)
    w_qkvg = width_gain * jax.random.normal(shared_keys[7], (BLOCKS, TOKEN_DIM, 4, TOKEN_DIM), jnp.float32)
    b_q = jax.random.normal(shared_keys[8], (BLOCKS, TOKEN_DIM), jnp.float32)
    w_o = 2.0 * width_gain * jax.random.normal(shared_keys[9], (BLOCKS, TOKEN_DIM, TOKEN_DIM), jnp.float32)
    up_down = jax.random.split(shared_keys[10], 2)
    w_up = width_gain * jax.random.normal(up_down[0], (BLOCKS, TOKEN_DIM, 2, HIDDEN_DIM), jnp.float32)
    w_down = 2.0 * hidden_gain * jax.random.normal(up_down[1], (BLOCKS, HIDDEN_DIM, TOKEN_DIM), jnp.float32)
    return {
        'token_act': token_act.astype(jnp.bfloat16),
        'token_cond': token_cond.astype(jnp.bfloat16),
        'pair_bias': pair_bias.astype(jnp.bfloat16),
        'token_mask': token_mask,
        'ada_scale': ada_scale,
        'ada_w': ada_w.astype(jnp.bfloat16),
        'ada_bias': ada_bias,
        'zero_w': zero_w.astype(jnp.bfloat16),
        'zero_b': zero_b,
        'w_qkvg': w_qkvg.astype(jnp.bfloat16),
        'b_q': b_q,
        'w_o': w_o.astype(jnp.bfloat16),
        'w_up': w_up.astype(jnp.bfloat16),
        'w_down': w_down.astype(jnp.bfloat16),
    }


def reference(token_act, token_cond, pair_bias, token_mask, ada_scale, ada_w, ada_bias, zero_w, zero_b, w_qkvg, b_q, w_o, w_up, w_down):
    row_count = SAMPLES * TOKENS
    head_shape = (SAMPLES, TOKENS, NUM_HEADS, HEAD_DIM)
    logit_scale = 1.0 / math.sqrt(HEAD_DIM)
    mask_add = (token_mask.astype(jnp.float32) - 1.0) * 1e9
    cond_flat = token_cond.reshape(row_count, COND_DIM)
    cond_normed = layer_norm(cond_flat.astype(jnp.float32))

    def block_step(act_flat, layer_args):
        (layer_scale, layer_ada_w, layer_ada_b, layer_zero_w, layer_zero_b, layer_qkvg, layer_bq, layer_wo, layer_up, layer_down, layer_bias) = layer_args
        out_gates = jax.nn.sigmoid(jnp.dot(cond_flat, layer_zero_w.reshape(COND_DIM, 2 * TOKEN_DIM), preferred_element_type=jnp.float32).reshape(row_count, 2, TOKEN_DIM) + layer_zero_b)
        act_f32 = act_flat.astype(jnp.float32)
        normed = ada_norm(act_f32, cond_normed, layer_scale[0], layer_ada_w[0], layer_ada_b[0])
        projected = jnp.dot(normed, layer_qkvg.reshape(TOKEN_DIM, 4 * TOKEN_DIM), preferred_element_type=jnp.float32).reshape(row_count, 4, TOKEN_DIM)
        query_rows = (projected[:, 0] + layer_bq).astype(jnp.bfloat16).reshape(head_shape)
        key_rows = projected[:, 1].astype(jnp.bfloat16).reshape(head_shape)
        value_rows = projected[:, 2].astype(jnp.bfloat16).reshape(head_shape)
        gate_heads = jax.nn.sigmoid(projected[:, 3])
        bias_f32 = layer_bias.astype(jnp.float32)

        def attend(operands):
            query_one, key_one, value_one = operands
            logits = jnp.einsum('qhc,khc->hqk', query_one.astype(jnp.float32), key_one.astype(jnp.float32)) * logit_scale + bias_f32 + mask_add
            attn_probs = jax.nn.softmax(logits, axis=-1).astype(jnp.bfloat16)
            return jnp.einsum('hqk,khc->qhc', attn_probs.astype(jnp.float32), value_one.astype(jnp.float32))

        mixed_heads = lax.map(attend, (query_rows, key_rows, value_rows)).reshape(row_count, TOKEN_DIM)
        heads_out = (gate_heads * mixed_heads).astype(jnp.bfloat16)
        attn_out = jnp.dot(heads_out, layer_wo, preferred_element_type=jnp.float32).astype(jnp.bfloat16).astype(jnp.float32)
        mid_f32 = (act_f32 + out_gates[:, 0] * attn_out).astype(jnp.bfloat16).astype(jnp.float32)
        normed_mid = ada_norm(mid_f32, cond_normed, layer_scale[1], layer_ada_w[1], layer_ada_b[1])
        hidden_pre = jnp.dot(normed_mid, layer_up.reshape(TOKEN_DIM, 2 * HIDDEN_DIM), preferred_element_type=jnp.float32).reshape(row_count, 2, HIDDEN_DIM)
        hidden = (jax.nn.silu(hidden_pre[:, 0]) * hidden_pre[:, 1]).astype(jnp.bfloat16)
        trans_out = jnp.dot(hidden, layer_down, preferred_element_type=jnp.float32).astype(jnp.bfloat16).astype(jnp.float32)
        act_next = (mid_f32 + out_gates[:, 1] * trans_out).astype(jnp.bfloat16)
        return act_next, None

    layer_stack = (ada_scale, ada_w, ada_bias, zero_w, zero_b, w_qkvg, b_q, w_o, w_up, w_down, pair_bias)
    final_act = lax.scan(block_step, token_act.reshape(row_count, TOKEN_DIM), layer_stack)[0]
    return final_act.reshape(SAMPLES, TOKENS, TOKEN_DIM)
```

```python
import math
import jax
import jax.numpy as jnp
from jax import lax
from jax.sharding import PartitionSpec as P

LN_EPS = 1e-5


def layer_norm(values_in):
    row_mean = jnp.mean(values_in, axis=-1, keepdims=True)
    centered = values_in - row_mean
    variance = jnp.mean(centered * centered, axis=-1, keepdims=True)
    return centered * lax.rsqrt(variance + LN_EPS)


def ada_norm(act_f32, cond_normed, scale_vec, weight, bias_vec):
    cond_in = (cond_normed * scale_vec).astype(jnp.bfloat16)
    gain = jnp.dot(cond_in, weight[:, 0], preferred_element_type=jnp.float32)
    shift = jnp.dot(cond_in, weight[:, 1], preferred_element_type=jnp.float32)
    return (jax.nn.sigmoid(gain + bias_vec) * layer_norm(act_f32) + shift).astype(jnp.bfloat16)


def solution(mesh):
    tp = mesh.shape['tp']

    def shard_body(token_act, token_cond, pair_bias, token_mask, ada_scale, ada_w, ada_bias, zero_w, zero_b, w_qkvg, b_q, w_o, w_up, w_down):
        samples, tokens, model_width = token_act.shape
        cond_dim = token_cond.shape[-1]
        heads_local = pair_bias.shape[1]
        local_width = w_qkvg.shape[-1]
        head_dim = local_width // heads_local
        own = samples // tp
        me = lax.axis_index('tp')
        act_own = lax.dynamic_slice_in_dim(token_act, me * own, own, 0)
        cond_own = lax.dynamic_slice_in_dim(token_cond, me * own, own, 0)
        row_count = own * tokens
        logit_scale = 1.0 / math.sqrt(head_dim)
        mask_add = (token_mask.astype(jnp.float32) - 1.0) * 1e9
        cond_flat = cond_own.reshape(row_count, cond_dim)
        cond_normed = layer_norm(cond_flat.astype(jnp.float32))
        act_flat = act_own.reshape(row_count, model_width)
        for layer in range(pair_bias.shape[0]):
            qkvg_all = lax.all_gather(w_qkvg[layer].reshape(model_width, -1), 'tp')
            bias_all = lax.all_gather(pair_bias[layer], 'tp')
            wo_all = lax.all_gather(w_o[layer], 'tp', tiled=True)
            bq_all = lax.all_gather(b_q[layer], 'tp')
            up_all = lax.all_gather(w_up[layer].reshape(model_width, -1), 'tp')
            down_all = lax.all_gather(w_down[layer], 'tp')
            out_gates = [jax.nn.sigmoid(jnp.dot(cond_flat, zero_w[layer, :, j], preferred_element_type=jnp.float32) + zero_b[layer, j]) for j in range(2)]
            act_f32 = act_flat.astype(jnp.float32)
            normed = ada_norm(act_f32, cond_normed, ada_scale[layer, 0], ada_w[layer, 0], ada_bias[layer, 0])
            heads_out = []
            for t in range(tp):
                projected = jnp.dot(normed, qkvg_all[t], preferred_element_type=jnp.float32).reshape(own, tokens, 4, heads_local, head_dim)
                query = (projected[:, :, 0] + bq_all[t].reshape(heads_local, head_dim)).astype(jnp.bfloat16)
                key = projected[:, :, 1].astype(jnp.bfloat16)
                value = projected[:, :, 2].astype(jnp.bfloat16)
                gate = jax.nn.sigmoid(projected[:, :, 3])
                logits = jnp.einsum('sqhc,skhc->shqk', query, key, preferred_element_type=jnp.float32) * logit_scale + bias_all[t] + mask_add
                probs = jax.nn.softmax(logits, axis=-1).astype(jnp.bfloat16)
                mixed = jnp.einsum('shqk,skhc->sqhc', probs, value, preferred_element_type=jnp.float32)
                heads_out.append((gate * mixed).astype(jnp.bfloat16).reshape(row_count, local_width))
            heads_cat = jnp.concatenate(heads_out, axis=-1)
            attn_out = jnp.dot(heads_cat, wo_all, preferred_element_type=jnp.float32).astype(jnp.bfloat16).astype(jnp.float32)
            mid_f32 = (act_f32 + out_gates[0] * attn_out).astype(jnp.bfloat16).astype(jnp.float32)
            normed_mid = ada_norm(mid_f32, cond_normed, ada_scale[layer, 1], ada_w[layer, 1], ada_bias[layer, 1])
            total = jnp.zeros((row_count, model_width), jnp.float32)
            for t in range(tp):
                hidden_pre = jnp.dot(normed_mid, up_all[t], preferred_element_type=jnp.float32).reshape(row_count, 2, -1)
                hidden = (jax.nn.silu(hidden_pre[:, 0]) * hidden_pre[:, 1]).astype(jnp.bfloat16)
                total += jnp.dot(hidden, down_all[t], preferred_element_type=jnp.float32)
            trans_out = total.astype(jnp.bfloat16).astype(jnp.float32)
            act_flat = (mid_f32 + out_gates[1] * trans_out).astype(jnp.bfloat16)
        return lax.all_gather(act_flat.reshape(own, tokens, model_width), 'tp', tiled=True)

    everywhere = P()
    in_specs = (P('dp', None, None), P('dp', None, None), P(None, 'tp', None, None), P(None), everywhere, everywhere, everywhere, everywhere, everywhere, P(None, None, None, 'tp'), P(None, 'tp'), P(None, 'tp', None), P(None, None, None, 'tp'), P(None, 'tp', None))
    return jax.shard_map(shard_body, mesh=mesh, in_specs=in_specs, out_specs=P('dp', None, None), check_vma=False)
```

```python
import functools
import math
import jax
import jax.numpy as jnp
from jax import lax
from jax.experimental import pallas as pl
from jax.experimental.pallas import tpu as pltpu
from jax.sharding import PartitionSpec as P

LN_EPS = 1e-5
LOG2E = 1.4426950408889634
MESH = pl.DeviceIdType.MESH
BF16 = jnp.bfloat16
F32 = jnp.float32
LANES = 128
CH = 1056
LA = 4
LAGS = (0, 1, 2, 3)
RB = 256
QB = 256
OUT_ROWS = 256
CORES = 2


def dot_nt(lhs, rhs):
    return lax.dot_general(lhs, rhs, (((1,), (1,)), ((), ())), preferred_element_type=F32)


def dot_nn(lhs, rhs):
    return lax.dot_general(lhs, rhs, (((1,), (0,)), ((), ())), preferred_element_type=F32)


def normed(values_in):
    row_mean = jnp.mean(values_in, axis=-1, keepdims=True)
    centered = values_in - row_mean
    variance = jnp.mean(centered * centered, axis=-1, keepdims=True)
    return centered * lax.rsqrt(variance + LN_EPS)


class Geometry:
    def __init__(self, mesh, act, cond, bias, w_qkvg, w_up):
        self.nx = mesh.shape['tp'] // CORES
        self.y_stride = len({d.coords[2] for d in mesh.devices.flat})
        self.samples, self.tokens, self.width = act
        self.cond_dim = cond[-1]
        self.layers, self.heads = bias[0], bias[1]
        self.lw = w_qkvg[-1]
        self.hd = self.lw // self.heads
        self.hu = w_up[-1]
        self.own = self.samples // mesh.shape['tp']
        self.ncol = self.width // LANES
        self.tcol = self.tokens // LANES
        self.q0 = 0
        self.b0 = self.q0 + self.ncol * 4 * self.lw
        self.o0 = self.b0 + self.heads * self.tcol * self.tokens
        self.u0 = self.o0 + self.ncol * self.lw
        self.d0 = self.u0 + self.ncol * 2 * self.hu
        self.lr = self.d0 + self.ncol * self.hu
        self.chunks = -(-self.layers * self.lr // CH)
        self.rows = self.chunks * CH
        self.per_layer = self.lr // CH + 1
        assert self.lw == 96 and self.hu == 192 and self.heads == 2 and self.nx == 4


def kernel(g, act_in, cond_in, bias_in, mask_in, ascale_in, ada_in, abias_in, zero_in, zbias_in, wq_in, bq_in, wo_in, up_in, down_in,
           out, buf, xbuf, pbuf, sbuf, obuf, hbuf, cbuf, lnbuf, adabuf, zerobuf, bqbuf, bmbuf, qbuf, kbuf, vbuf, gbuf,
           s_loc, s_act, s_ada, send, ra, rb, rc, rd, s_bq, r_bq, sx, rx, sp, rp, osend, o_p0, o_a, o_p1, o_d, o_p2):
    nx, own, T, D = g.nx, g.own, g.tokens, g.width
    tp = lax.axis_index('tp')
    dp = lax.axis_index('dp')
    x = tp // CORES
    c = lax.rem(tp, CORES)
    xp = lax.rem(x + 1, nx)
    xm = lax.rem(x + nx - 1, nx)
    xo = lax.rem(x + 2, nx)
    dev_p, dev_m, dev_o = ({'tp': v * CORES + c} for v in (xp, xm, xo))
    dev_c = {'tp': x * CORES + 1 - c}
    pz = lax.rem(dp, 2)
    py = lax.rem(dp // g.y_stride, 2)
    dev_z = {'dp': dp + 1 - 2 * pz}
    dev_y = {'dp': dp + g.y_stride * (1 - 2 * py)}

    def remote(src, dst, s_sem, r_sem, dev):
        return pltpu.make_async_remote_copy(src, dst, s_sem, r_sem, device_id=dev, device_id_type=MESH)

    def wait_like(ref, sem):
        pltpu.make_async_copy(ref, ref, sem).wait()

    lw, hu = g.lw, g.hu
    half = hu - LANES
    q_parts = ((0, 0, lw, 0), (3, 0, 32, lw), (1, 0, lw, LANES), (3, 32, 32, LANES + lw), (2, 0, lw, 2 * LANES), (3, 64, 32, 2 * LANES + lw))
    u_parts = ((0, 0, LANES, 0), (0, LANES, half, LANES), (1, LANES, half, LANES + half), (1, 0, LANES, 2 * LANES))

    def load_layer(l):
        def put(src, off, n):
            pltpu.make_async_copy(src, buf.at[x, pl.ds(l * g.lr + off, n)], s_loc.at[l]).start()
        for j in range(g.ncol):
            col = pl.ds(j * LANES, LANES)
            for f, r0, n, off in q_parts:
                put(wq_in.at[l, f, pl.ds(r0, n), col], g.q0 + j * 4 * lw + off, n)
        for h in range(g.heads):
            for j in range(g.tcol):
                put(bias_in.at[l, h, :, pl.ds(j * LANES, LANES)], g.b0 + (h * g.tcol + j) * T, T)
        for j in range(g.ncol):
            col = pl.ds(j * LANES, LANES)
            put(wo_in.at[l, :, col], g.o0 + j * lw, lw)
            for f, r0, n, off in u_parts:
                put(up_in.at[l, f, pl.ds(r0, n), col], g.u0 + j * 2 * hu + off, n)
            put(down_in.at[l, :, col], g.d0 + j * hu, hu)

    load_layer(0)
    mine = tp * own
    act_cp = pltpu.make_async_copy(act_in.at[pl.ds(mine, own)], out.at[pl.ds(mine, own)], s_act.at[0])
    cond_cp = pltpu.make_async_copy(cond_in.at[pl.ds(mine, own)], cbuf, s_act.at[1])
    ada_cp = pltpu.make_async_copy(ada_in, adabuf, s_ada.at[0])
    zero_cp = pltpu.make_async_copy(zero_in, zerobuf, s_ada.at[1])
    bq_cp = pltpu.make_async_copy(bq_in, bqbuf.at[x], s_act.at[2])
    for cp in (act_cp, cond_cp, bq_cp, ada_cp, zero_cp):
        cp.start()
    for l in range(1, g.layers):
        load_layer(l)

    barrier = pltpu.get_barrier_semaphore()
    devs = (dev_p, dev_m, dev_o, dev_c, dev_z, dev_y)
    for d in devs:
        pl.semaphore_signal(barrier, inc=1, device_id=d, device_id_type=MESH)
    pad = g.rows - g.layers * g.lr
    if pad:
        buf[x, pl.ds(g.layers * g.lr, pad), :] = jnp.zeros((pad, LANES), BF16)
    pl.semaphore_wait(barrier, len(devs))
    for l in range(g.layers):
        wait_like(buf.at[x, pl.ds(l * g.lr, g.lr)], s_loc.at[l])

    Q = CH // 4
    g0 = 2 * py + pz
    gy = 2 * (1 - py) + pz
    gz = 2 * py + 1 - pz
    gd = 2 * (1 - py) + 1 - pz

    def piece(blk, k, part):
        return buf.at[blk, pl.ds(pl.multiple_of(k * CH + part * Q, 8), Q)]

    def push(blk, k, part, dev, r_sem):
        r = piece(blk, k, part)
        remote(r, r, send, r_sem, dev).start()

    def await_quarters(n, sem):
        wait_like(buf.at[0, pl.ds(0, n * Q)], sem)

    def first(k):
        push(x, k, g0, dev_p, ra.at[k])
        push(x, k, g0, dev_m, ra.at[k])

    def stage1(k):
        await_quarters(2, ra.at[k])
        push(xm, k, g0, dev_p, rd.at[k])
        for blk in (xm, xp):
            push(blk, k, g0, dev_y, rb.at[k])
            push(blk, k, g0, dev_z, rb.at[k])

    def stage2(k):
        await_quarters(4, rb.at[k])
        push(xm, k, gy, dev_p, rd.at[k])
        push(xp, k, gz, dev_m, rd.at[k])
        push(xm, k, gz, dev_y, rc.at[k])
        push(xp, k, gy, dev_z, rc.at[k])

    def stage3(k):
        await_quarters(2, rc.at[k])
        push(xp, k, gd, dev_m, rd.at[k])

    def stage4(k):
        await_quarters(4, rd.at[k])

    K = g.chunks
    last_tick = K + LAGS[-1]

    def tick(t):
        @pl.when(t + LA < K)
        def _():
            first(t + LA)
        for lag, stage in zip(LAGS, (stage1, stage2, stage3, stage4)):
            @pl.when((t >= lag) & (t - lag < K))
            def _(lag=lag, stage=stage):
                stage(t - lag)

    def ahead(k, carry):
        first(k)
        return carry
    lax.fori_loop(0, LA, ahead, 0)

    carried = max(0, -(-g.lr // CH) + LAGS[-1] - g.per_layer)

    def reached(l, rel):
        return jnp.minimum(jnp.maximum(l * g.per_layer + rel, jnp.where(l > 0, l * g.per_layer + carried, 0)), last_tick)

    def advance(l, lo, hi):
        def body(t, carry):
            tick(t)
            return carry
        lax.fori_loop(reached(l, lo), reached(l, hi), body, 0)

    def need(rows_end, lag):
        return -(-rows_end // CH) + lag

    bq_cp.wait()
    for d in (dev_p, dev_m, dev_o):
        remote(bqbuf.at[x], bqbuf.at[x], s_bq, r_bq, d).start()
    act_cp.wait()
    cond_cp.wait()

    lane = lax.broadcasted_iota(jnp.int32, (1, LANES), 1)
    hd = g.hd
    mask_add = (mask_in[...].astype(F32) - 1.0) * (1e9 * LOG2E)
    scale2 = LOG2E / math.sqrt(hd)

    def cond_rows(i, r):
        rows = pl.ds(r * RB, RB)
        lnbuf[i, rows, :] = normed(cbuf[i, rows, :].astype(F32))

    nrb = T // RB
    for i in range(own):
        for r in range(nrb):
            cond_rows(i, r)
    ada_cp.wait()
    zero_cp.wait()

    def ada_rows(l, j, i, r):
        rows = pl.ds(pl.multiple_of(r * RB, RB), RB)
        lj = l * 2 + j
        c_in = (lnbuf[i, rows, :] * ascale_in[lj]).astype(BF16)
        gain = jax.nn.sigmoid(dot_nn(c_in, adabuf[lj, 0]) + abias_in[lj])
        shift = dot_nn(c_in, adabuf[lj, 1])
        xbuf[i, rows, :] = (gain * normed(out[mine + i, rows, :].astype(F32)) + shift).astype(BF16)

    def ada_sample(l, j, i):
        def body(r, carry):
            ada_rows(l, j, i, r)
            return carry
        lax.fori_loop(0, nrb, body, 0)
        remote(xbuf.at[i], xbuf.at[own + i], sx.at[i], rx.at[i], dev_c).start()

    def resid_rows(l, j, i, r, part_of):
        rows = pl.ds(pl.multiple_of(r * RB, RB), RB)
        lj = l * 2 + j
        total = (part_of(l, i, rows) + pbuf[i, rows, :].astype(F32)).astype(BF16).astype(F32)
        gate = jax.nn.sigmoid(dot_nn(cbuf[i, rows, :], zerobuf[lj]) + zbias_in[lj])
        out[mine + i, rows, :] = (out[mine + i, rows, :].astype(F32) + gate * total).astype(BF16)

    def resid_sample(l, j, i, part_of):
        wait_like(pbuf.at[i], rp.at[i])
        def body(r, carry):
            resid_rows(l, j, i, r, part_of)
            return carry
        lax.fori_loop(0, nrb, body, 0)

    def part_sample(l, i, part_of):
        def body(r, carry):
            rows = pl.ds(pl.multiple_of(r * RB, RB), RB)
            sbuf[i, rows, :] = part_of(l, own + i, rows).astype(BF16)
            return carry
        lax.fori_loop(0, nrb, body, 0)
        remote(sbuf.at[i], pbuf.at[i], sp.at[i], rp.at[i], dev_c).start()

    def flat(s, l, off, n):
        return buf[s, pl.ds(pl.multiple_of(l * g.lr + off, 8), n), :]

    def bias_prep(l, s):
        for h in range(g.heads):
            for j in range(g.tcol):
                col = pl.ds(j * LANES, LANES)
                bmbuf[h, :, col] = flat(s, l, g.b0 + (h * g.tcol + j) * T, T).astype(F32) * LOG2E + mask_add[:, j * LANES:(j + 1) * LANES]

    def unit(l, s, i):
        w = jnp.concatenate([flat(s, l, g.q0 + j * 4 * lw, 4 * lw) for j in range(g.ncol)], axis=1)
        for r in range(T // QB):
            rows = pl.ds(r * QB, QB)
            proj = dot_nt(xbuf[i, rows, :], w)
            pa, pb, pc = (proj[:, v * LANES:(v + 1) * LANES] for v in range(3))
            qbuf[rows, :] = (pa + bqbuf[s, pl.ds(l, 1), :]).astype(BF16)
            kbuf[rows, :] = pb.astype(BF16)
            vbuf[rows, :] = jnp.where(lane < lw, pc, 1.0).astype(BF16)
            gate = jnp.where(lane < 32, pltpu.roll(pa, 32, 1), jnp.where(lane < 64, pltpu.roll(pb, 64, 1), pltpu.roll(pc, 96, 1)))
            gbuf[rows, :] = jnp.where(lane < lw, jax.nn.sigmoid(gate), 0.0)
        keys = kbuf[...]
        values = vbuf[...]
        for r in range(T // QB):
            rows = pl.ds(r * QB, QB)
            mixed = []
            for h in range(g.heads):
                q = jnp.where((lane >= h * hd) & (lane < (h + 1) * hd), qbuf[rows, :], jnp.zeros((), BF16))
                z = dot_nt(q, keys) * scale2 + bmbuf[h, rows, :]
                e = jnp.exp2(z - jnp.max(z, axis=-1, keepdims=True)).astype(BF16)
                o = dot_nn(e, values)
                mixed.append(o * (1.0 / o[:, lw:lw + 1]))
            obuf[i, s, rows, :] = (jnp.where(lane < hd, mixed[0], mixed[1]) * gbuf[rows, :]).astype(BF16)

    def attend(l, s, lo, hi):
        def body(i, carry):
            unit(l, s, i)
            return carry
        lax.fori_loop(lo, hi, body, 0)

    def attn_part(l, i, rows):
        lhs = jnp.concatenate([obuf[i, s, rows, :] for s in range(nx)], axis=1)
        zpad = jnp.zeros((LANES - lw, LANES), BF16)
        rhs = jnp.concatenate([jnp.concatenate([v for s in range(nx) for v in (flat(s, l, g.o0 + j * lw, lw), zpad)], axis=0) for j in range(g.ncol)], axis=1)
        return dot_nn(lhs, rhs)

    def up_sample(l, i):
        for r in range(T // RB):
            rows = pl.ds(r * RB, RB)
            y = xbuf[i, rows, :]
            for p in range(nx // 2):
                mids = []
                for e in range(2):
                    s = 2 * p + e
                    w = jnp.concatenate([flat(s, l, g.u0 + j * 2 * hu, 2 * hu) for j in range(g.ncol)], axis=1)
                    u = dot_nt(y, w)
                    ua, ub, uc = (u[:, v * LANES:(v + 1) * LANES] for v in range(3))
                    side = (3 * p + 2 * e) * LANES
                    hbuf[i, rows, side:side + LANES] = (jax.nn.silu(ua) * uc).astype(BF16)
                    act = jax.nn.silu(ub)
                    mids.append(act * pltpu.roll(ub, half, 1) if e == 0 else pltpu.roll(act, half, 1) * ub)
                mid = (3 * p + 1) * LANES
                hbuf[i, rows, mid:mid + LANES] = jnp.where(lane < half, mids[0], mids[1]).astype(BF16)

    def trans_part(l, i, rows):
        cols = []
        for j in range(g.ncol):
            v = []
            for p in range(nx // 2):
                v.append(flat(2 * p, l, g.d0 + j * hu, hu))
                v.append(flat(2 * p + 1, l, g.d0 + j * hu + LANES, half))
                v.append(flat(2 * p + 1, l, g.d0 + j * hu, LANES))
            cols.append(jnp.concatenate(v, axis=0))
        return dot_nn(hbuf[i, rows, :], jnp.concatenate(cols, axis=1))

    def sends_done(ref, sem):
        for i in range(own):
            wait_like(ref.at[i], sem.at[i])

    t_q = need(g.b0, LAGS[2])
    t_near = need(g.o0, LAGS[2])
    t_far = need(g.u0, LAGS[3])
    t_up = need(g.d0, LAGS[3])
    t_down = need(g.lr, LAGS[3])

    def layer(l, carry):
        ada_sample(l, 0, 0)
        advance(l, 0, 1)
        ada_sample(l, 0, 1)
        advance(l, 1, 2)
        bias_prep(l, x)
        attend(l, x, 0, own)
        advance(l, 2, 3)
        for i in range(own):
            wait_like(xbuf.at[own + i], rx.at[i])
        attend(l, x, own, 2 * own)
        advance(l, 3, t_near)

        @pl.when(l == 0)
        def _():
            wait_like(bqbuf.at[pl.ds(0, nx - 1)], r_bq)
        bias_prep(l, xm)
        attend(l, xm, 0, 2 * own)
        advance(l, t_near, t_near + 1)
        bias_prep(l, xp)
        attend(l, xp, 0, 2 * own)
        advance(l, t_near + 1, t_far)
        bias_prep(l, xo)
        attend(l, xo, 0, 2 * own)
        sends_done(xbuf, sx)
        for i in range(own):
            part_sample(l, i, attn_part)
        for i in range(own):
            resid_sample(l, 0, i, attn_part)
        for i in range(own):
            ada_sample(l, 1, i)
        sends_done(sbuf, sp)
        advance(l, t_far, t_up)
        def up_body(i, carry):
            up_sample(l, i)
            return carry
        lax.fori_loop(0, own, up_body, 0)
        for i in range(own):
            wait_like(xbuf.at[own + i], rx.at[i])
        lax.fori_loop(own, 2 * own, up_body, 0)
        advance(l, t_up, t_down)
        for i in range(own):
            part_sample(l, i, trans_part)
        sends_done(xbuf, sx)
        for i in range(own):
            resid_sample(l, 1, i, trans_part)
        sends_done(sbuf, sp)
        return carry

    lax.fori_loop(0, g.layers, layer, 0)

    PR = OUT_ROWS
    pieces = [(s, h) for s in range(own) for h in range(T // PR)]
    tpp, tpm, tpo = (v * CORES + c for v in (xp, xm, xo))

    def orow(blk, p, lo=0, n=PR):
        s, h = pieces[p]
        return out.at[blk * own + s, pl.ds(h * PR + lo, n)]

    def opush(r, dev, sem):
        remote(r, r, osend, sem, dev).start()

    def oawait(halves, sem):
        wait_like(out.at[0, pl.ds(0, halves * PR // 2)], sem)

    for p in range(len(pieces)):
        opush(orow(tp, p), dev_p, o_a.at[p])
        opush(orow(tp, p), dev_m, o_a.at[p])
        opush(orow(tp, p), dev_c, o_p0.at[p])
    for p in range(len(pieces)):
        oawait(4, o_a.at[p])
        opush(orow(tpm, p, 0, PR // 2), dev_p, o_d.at[p])
        opush(orow(tpp, p, PR // 2, PR // 2), dev_m, o_d.at[p])
        opush(orow(tpm, p), dev_c, o_p1.at[p])
        opush(orow(tpp, p), dev_c, o_p1.at[p])
    for p in range(len(pieces)):
        oawait(2, o_d.at[p])
        opush(orow(tpo, p), dev_c, o_p2.at[p])
    for p in range(len(pieces)):
        oawait(2, o_p0.at[p])
        oawait(4, o_p1.at[p])
        oawait(2, o_p2.at[p])
    wait_like(out.at[pl.ds(0, 7 * own)], osend)
    wait_like(buf.at[pl.ds(0, 3)], send)
    wait_like(bqbuf.at[pl.ds(0, nx - 1)], s_bq)


def finish(src, dst, sem):
    cp = pltpu.make_async_copy(src, dst, sem)
    cp.start()
    cp.wait()


def solution(mesh):
    def body(token_act, token_cond, pair_bias, token_mask, ada_scale, ada_w, ada_bias, zero_w, zero_b, w_qkvg, b_q, w_o, w_up, w_down):
        g = Geometry(mesh, token_act.shape, token_cond.shape, pair_bias.shape, w_qkvg.shape, w_up.shape)
        L, D, C, T, own, nx = g.layers, g.width, g.cond_dim, g.tokens, g.own, g.nx
        ada = ada_w.transpose(0, 1, 3, 2, 4).reshape(2 * L, 2, C, D)
        zero = zero_w.transpose(0, 2, 1, 3).reshape(2 * L, C, D)
        bq = jnp.pad(b_q, ((0, 8 - L), (0, LANES - g.lw)))
        vm = pl.BlockSpec(memory_space=pltpu.VMEM)
        hbm = pl.BlockSpec(memory_space=pl.ANY)
        dma = pltpu.SemaphoreType.DMA
        npc = own * (T // OUT_ROWS)
        K = g.chunks
        gathered = pl.pallas_call(
            functools.partial(kernel, g),
            out_shape=pltpu.VMEM(token_act.shape, BF16),
            in_specs=[hbm, hbm, hbm, vm, vm, hbm, vm, hbm, vm, hbm, hbm, hbm, hbm, hbm],
            out_specs=vm,
            scratch_shapes=[
                pltpu.VMEM((nx, g.rows, LANES), BF16),
                pltpu.VMEM((2 * own, T, D), BF16),
                pltpu.VMEM((own, T, D), BF16),
                pltpu.VMEM((own, T, D), BF16),
                pltpu.VMEM((2 * own, nx, T, LANES), BF16),
                pltpu.VMEM((2 * own, T, nx * g.hu), BF16),
                pltpu.VMEM((own, T, C), BF16),
                pltpu.VMEM((own, T, C), F32),
                pltpu.VMEM((2 * L, 2, C, D), BF16),
                pltpu.VMEM((2 * L, C, D), BF16),
                pltpu.VMEM((nx, 8, LANES), F32),
                pltpu.VMEM((g.heads, T, T), F32),
                pltpu.VMEM((T, LANES), BF16),
                pltpu.VMEM((T, LANES), BF16),
                pltpu.VMEM((T, LANES), BF16),
                pltpu.VMEM((T, LANES), F32),
                dma((L,)), dma((3,)), dma((2,)), dma,
                dma((K,)), dma((K,)), dma((K,)), dma((K,)),
                dma, dma, dma((own,)), dma((own,)), dma((own,)), dma((own,)),
                dma, dma((npc,)), dma((npc,)), dma((npc,)), dma((npc,)), dma((npc,)),
            ],
            compiler_params=pltpu.CompilerParams(collective_id=0, has_side_effects=True, vmem_limit_bytes=50 << 20),
            name='blocks',
        )(token_act, token_cond, pair_bias, token_mask.reshape(1, T), ada_scale.reshape(2 * L, 1, C), ada, ada_bias.reshape(2 * L, 1, D),
          zero, zero_b.reshape(2 * L, 1, D), w_qkvg.transpose(0, 2, 3, 1), bq, w_o, w_up.transpose(0, 2, 3, 1), w_down)
        gathered = pltpu.with_memory_space_constraint(gathered, pltpu.VMEM)
        return pl.pallas_call(
            finish,
            out_shape=jax.ShapeDtypeStruct(token_act.shape, BF16),
            in_specs=[vm],
            out_specs=pl.BlockSpec(memory_space=pltpu.HBM),
            scratch_shapes=[dma],
            compiler_params=pltpu.CompilerParams(vmem_limit_bytes=1 << 20),
            name='finish',
        )(gathered)

    everywhere = P()
    in_specs = (P('dp', None, None), P('dp', None, None), P(None, 'tp', None, None), P(None), everywhere, everywhere, everywhere, everywhere, everywhere, P(None, None, None, 'tp'), P(None, 'tp'), P(None, 'tp', None), P(None, None, None, 'tp'), P(None, 'tp', None))
    return jax.shard_map(body, mesh=mesh, in_specs=in_specs, out_specs=P('dp', None, None), check_vma=False)
```

```python
import functools
import math
import jax
import jax.numpy as jnp
from jax import lax
from jax.experimental import pallas as pl
from jax.experimental.pallas import tpu as pltpu
from jax.sharding import PartitionSpec as P

LN_EPS = 1e-5
LOG2E = 1.4426950408889634
MESH = pl.DeviceIdType.MESH
BF16 = jnp.bfloat16
F32 = jnp.float32
LANES = 128
CH = 1056
LA = 4
TAIL_TICKS = 7
RELAY_AT = 2
HELD = 2
LAGS = (0, 1, 2)
RB = 512
OUT_ROWS = 256
CORES = 2


def dot_nt(lhs, rhs):
    return lax.dot_general(lhs, rhs, (((1,), (1,)), ((), ())), preferred_element_type=F32)


def dot_nn(lhs, rhs):
    return lax.dot_general(lhs, rhs, (((1,), (0,)), ((), ())), preferred_element_type=F32)


def normed(values_in):
    row_mean = jnp.mean(values_in, axis=-1, keepdims=True)
    centered = values_in - row_mean
    variance = jnp.mean(centered * centered, axis=-1, keepdims=True)
    return centered * lax.rsqrt(variance + LN_EPS)


class Geometry:
    def __init__(self, mesh, act, cond, bias, w_qkvg, w_up):
        self.nx = mesh.shape['tp'] // CORES
        self.y_stride = len({d.coords[2] for d in mesh.devices.flat})
        self.samples, self.tokens, self.width = act
        self.cond_dim = cond[-1]
        self.layers, self.heads = bias[0], bias[1]
        self.lw = w_qkvg[-1]
        self.hd = self.lw // self.heads
        self.hu = w_up[-1]
        self.own = self.samples // mesh.shape['tp']
        self.ncol = self.width // LANES
        self.tcol = self.tokens // LANES
        self.q0 = 0
        self.b0 = self.q0 + self.ncol * 4 * self.lw
        self.o0 = self.b0 + self.heads * self.tcol * self.tokens
        self.u0 = self.o0 + self.ncol * self.lw
        self.d0 = self.u0 + self.ncol * 2 * self.hu
        self.lr = self.d0 + self.ncol * self.hu
        self.flat_rows = self.layers * self.lr - self.o0
        self.chunks = -(-self.flat_rows // CH)
        self.rows = self.chunks * CH
        assert self.lw == 96 and self.hu == 192 and self.heads == 2 and self.nx == 4 and self.layers == 2 and self.own == 2


def kernel(g, act_in, cond_in, bias_in, mask_in, ascale_in, ada_in, abias_in, zero_in, zbias_in, wq_in, bq_in, wo_in, up_in, down_in,
           out, buf, qb0, xbuf, abuf, pbuf, obuf, hbuf, cring, cbuf, lnbuf, adabuf, zerobuf, bqbuf, bmbuf, qa, ka, va, ga, qb, kb, vb, gb,
           s_loc, s_act, s_ada, s_in, send, ra, rb, rc, rd, s_bq, r_bq, sx0, rx0, s_o, r_o, r_rel, sx, rx, sp, rp, osend, o_p0, o_a, o_p1, o_d, o_p2):
    nx, own, T, D = g.nx, g.own, g.tokens, g.width
    lw, hu, hd = g.lw, g.hu, g.hd
    half = hu - LANES
    tp = lax.axis_index('tp')
    dp = lax.axis_index('dp')
    x = tp // CORES
    c = lax.rem(tp, CORES)
    xp = lax.rem(x + 1, nx)
    xm = lax.rem(x + nx - 1, nx)
    xo = lax.rem(x + 2, nx)
    dev_p, dev_m, dev_o = ({'tp': v * CORES + c} for v in (xp, xm, xo))
    dev_c = {'tp': x * CORES + 1 - c}
    pz = lax.rem(dp, 2)
    py = lax.rem(dp // g.y_stride, 2)
    dev_z = {'dp': dp + 1 - 2 * pz}
    dev_y = {'dp': dp + g.y_stride * (1 - 2 * py)}
    mine = tp * own

    def remote(src, dst, s_sem, r_sem, dev):
        return pltpu.make_async_remote_copy(src, dst, s_sem, r_sem, device_id=dev, device_id_type=MESH)

    def wait_like(ref, sem):
        pltpu.make_async_copy(ref, ref, sem).wait()

    barrier = pltpu.get_barrier_semaphore()
    devs = (dev_p, dev_m, dev_o, dev_c, dev_z, dev_y)
    for d in devs:
        pl.semaphore_signal(barrier, inc=1, device_id=d, device_id_type=MESH)

    steps = nx * own

    def chip_of(n):
        near = jnp.where(lax.rem(n, 2) == 0, 1, nx - 1)
        return lax.rem(x + jnp.where(n < own, 2, jnp.where(n < 3 * own, near, 0)), nx)

    def pair_of(n):
        return jnp.where((n < own) | (n >= 3 * own), lax.rem(n, own), (n - own) // 2)

    def sample_of(n, core):
        return chip_of(n) * (CORES * own) + pair_of(n) * CORES + core

    def load_sample(n):
        slot = lax.rem(n, 2 * own)
        pltpu.make_async_copy(act_in.at[sample_of(n, c)], hbuf.at[slot], s_in.at[0, slot]).start()
        pltpu.make_async_copy(cond_in.at[sample_of(n, c)], cring.at[slot], s_in.at[1, slot]).start()

    load_sample(0)
    ada_cps = [pltpu.make_async_copy(ada_in.at[v], adabuf.at[v], s_ada.at[v]) for v in range(2 * g.layers)]
    zero_cps = [pltpu.make_async_copy(zero_in.at[v], zerobuf.at[v], s_ada.at[2 * g.layers + v]) for v in range(2 * g.layers)]
    ada_cps[0].start()

    q_parts = ((0, 0, lw, 0), (3, 0, 32, lw), (1, 0, lw, LANES), (3, 32, 32, LANES + lw), (2, 0, lw, 2 * LANES), (3, 64, 32, 2 * LANES + lw))
    u_parts = ((0, 0, LANES, 0), (0, LANES, half, LANES), (1, LANES, half, LANES + half), (1, 0, LANES, 2 * LANES))

    def load_attn(l, place, sem):
        for j in range(g.ncol):
            for f, r0, n, off in q_parts:
                pltpu.make_async_copy(wq_in.at[l, f, pl.ds(r0, n), pl.ds(j * LANES, LANES)], place(g.q0 + j * 4 * lw + off, n), sem).start()
        for h in range(g.heads):
            for j in range(g.tcol):
                pltpu.make_async_copy(bias_in.at[l, h, :, pl.ds(j * LANES, LANES)], place(g.b0 + (h * g.tcol + j) * T, T), sem).start()

    def load_rest(l, place, sem):
        for j in range(g.ncol):
            col = pl.ds(j * LANES, LANES)
            pltpu.make_async_copy(wo_in.at[l, :, col], place(g.o0 + j * lw, lw), sem).start()
            for f, r0, n, off in u_parts:
                pltpu.make_async_copy(up_in.at[l, f, pl.ds(r0, n), col], place(g.u0 + j * 2 * hu + off, n), sem).start()
            pltpu.make_async_copy(down_in.at[l, :, col], place(g.d0 + j * hu, hu), sem).start()

    def own_rows(l):
        return lambda off, n: buf.at[x, pl.ds(l * g.lr - g.o0 + off, n)]

    load_rest(0, own_rows(0), s_loc.at[1])
    act_cp = pltpu.make_async_copy(act_in.at[pl.ds(mine, own)], abuf, s_act.at[0])
    cond_cp = pltpu.make_async_copy(cond_in.at[pl.ds(mine, own)], cbuf, s_act.at[1])
    bqbuf[x] = jnp.zeros((8, LANES), F32)
    bqbuf[x, pl.ds(0, g.layers), pl.ds(0, lw)] = bq_in[...]

    pad = g.rows - g.flat_rows
    if pad:
        buf[x, pl.ds(g.flat_rows, pad), :] = jnp.zeros((pad, LANES), BF16)

    Q = CH // 4
    g0 = 2 * py + pz
    gy = 2 * (1 - py) + pz
    gz = 2 * py + 1 - pz
    gd = 2 * (1 - py) + 1 - pz

    def push(blk, k, part, dev, r_sem):
        r = buf.at[blk, pl.ds(pl.multiple_of(k * CH + part * Q, 8), Q)]
        remote(r, r, send, r_sem, dev).start()

    def await_quarters(n, sem):
        wait_like(buf.at[0, pl.ds(0, n * Q)], sem)

    def first(k):
        push(x, k, g0, dev_p, ra.at[k])
        push(x, k, g0, dev_m, ra.at[k])

    def stage1(k):
        await_quarters(2, ra.at[k])
        push(xm, k, g0, dev_p, rd.at[k])
        for blk in (xm, xp):
            push(blk, k, g0, dev_y, rb.at[k])
            push(blk, k, g0, dev_z, rb.at[k])

    def stage2(k):
        await_quarters(4, rb.at[k])
        push(xm, k, gy, dev_p, rd.at[k])
        push(xp, k, gz, dev_m, rd.at[k])
        push(xm, k, gz, dev_y, rc.at[k])
        push(xp, k, gy, dev_z, rc.at[k])

    def stage3(k):
        await_quarters(2, rc.at[k])
        push(xp, k, gd, dev_m, rd.at[k])

    def stage4(k):
        await_quarters(4, rd.at[k])

    K = g.chunks

    def tick(t):
        @pl.when(t + LA < K)
        def _():
            first(t + LA)
        for lag, stage in zip(LAGS, (stage1, stage2, stage3)):
            @pl.when((t >= lag) & (t - lag < K))
            def _(lag=lag, stage=stage):
                stage(t - lag)

    def need(rows_end, lag):
        return -(-(rows_end - g.o0) // CH) + lag

    lane = lax.broadcasted_iota(jnp.int32, (1, LANES), 1)
    mask_add = (mask_in[...].astype(F32) - 1.0) * (1e9 * LOG2E)
    scale2 = LOG2E / math.sqrt(hd)

    def modulated(l, j, cond_ln, act_f32):
        c_in = (cond_ln * ascale_in[l, pl.ds(j, 1), :]).astype(BF16)
        gain = jax.nn.sigmoid(dot_nn(c_in, adabuf[l * 2 + j, 0]) + abias_in[l, pl.ds(j, 1), :])
        shift = dot_nn(c_in, adabuf[l * 2 + j, 1])
        return (gain * normed(act_f32) + shift).astype(BF16)

    def row_blocks(body):
        for r in range(T // RB):
            body(pl.ds(r * RB, RB))

    def ada_sample(l, j, i):
        def rows_body(rows):
            xbuf[i, rows, :] = modulated(l, j, lnbuf[i, rows, :], abuf[i, rows, :].astype(F32))
        row_blocks(rows_body)
        remote(xbuf.at[i], xbuf.at[own + i], sx.at[i], rx.at[i], dev_c).start()

    stage0 = 2 * own * nx

    def relay_box(v):
        return xbuf.at[v, :, pl.ds(0, LANES)]

    def sent_part(i):
        return obuf.at[pl.ds(stage0 + i * g.ncol, g.ncol)]

    def got_part(i):
        return pbuf.at[pl.ds(i * g.ncol, g.ncol)]

    def resid_sample(l, j, i, part_of):
        rows = pl.ds(0, T)
        ours = part_of(l, i, rows)
        gate = jax.nn.sigmoid(dot_nn(cbuf[i], zerobuf[l * 2 + j]) + zbias_in[l, pl.ds(j, 1), :])
        wait_like(got_part(i), rp.at[i])
        theirs = jnp.concatenate([pbuf[i * g.ncol + v] for v in range(g.ncol)], axis=1)
        act = (abuf[i].astype(F32) + gate * (ours + theirs.astype(F32)).astype(BF16).astype(F32)).astype(BF16)
        abuf[i] = act
        if j == 1:
            out[mine + i] = act

    def part_sample(l, i, part_of):
        def rows_body(rows):
            part = part_of(l, own + i, rows).astype(BF16)
            for v in range(g.ncol):
                obuf[stage0 + i * g.ncol + v, rows, :] = part[:, v * LANES:(v + 1) * LANES]
        row_blocks(rows_body)
        remote(sent_part(i), got_part(i), sp.at[i], rp.at[i], dev_c).start()

    def flat(s, l, off, n):
        return buf[s, pl.ds(pl.multiple_of(l * g.lr - g.o0 + off, 8), n), :]

    def bias_prep(rows_of):
        for h in range(g.heads):
            for j in range(g.tcol):
                col = pl.ds(j * LANES, LANES)
                bmbuf[h, :, col] = rows_of(g.b0 + (h * g.tcol + j) * T, T).astype(F32) * LOG2E + mask_add[:, j * LANES:(j + 1) * LANES]

    def project(slot, x_rows, rows_of, q_bias):
        qs, ks, vs, gs = slot
        w = jnp.concatenate([rows_of(g.q0 + j * 4 * lw, 4 * lw) for j in range(g.ncol)], axis=1)
        proj = dot_nt(x_rows, w)
        pa, pb, pc = (proj[:, v * LANES:(v + 1) * LANES] for v in range(3))
        qs[...] = (pa + q_bias).astype(BF16)
        ks[...] = pb.astype(BF16)
        vs[...] = jnp.where(lane < lw, pc, 1.0).astype(BF16)
        gate = jnp.where(lane < 32, pltpu.roll(pa, 32, 1), jnp.where(lane < 64, pltpu.roll(pb, 64, 1), pltpu.roll(pc, 96, 1)))
        gs[...] = jnp.where(lane < lw, jax.nn.sigmoid(gate), 0.0)

    def attend(slot, o_ref):
        qs, ks, vs, gs = slot
        q = qs[...]
        zero = jnp.zeros((), BF16)
        both = jnp.concatenate([jnp.where((lane >= h * hd) & (lane < (h + 1) * hd), q, zero) for h in range(g.heads)], axis=0)
        z = dot_nt(both, ks[...]) * scale2 + jnp.concatenate([bmbuf[h] for h in range(g.heads)], axis=0)
        e = jnp.exp2(z - jnp.max(z, axis=-1, keepdims=True)).astype(BF16)
        o = dot_nn(e, vs[...])
        o = o * (1.0 / o[:, lw:lw + 1])
        o_ref[...] = (jnp.where(lane < hd, o[:T], o[T:]) * gs[...]).astype(BF16)

    slot_a = (qa, ka, va, ga)
    slot_b = (qb, kb, vb, gb)

    def ada_first(n):
        slot = lax.rem(n, 2 * own)
        s = sample_of(n, c)
        wait_like(hbuf.at[slot], s_in.at[0, slot])
        wait_like(cring.at[slot], s_in.at[1, slot])
        def rows_body(rows):
            out[s, rows, :] = modulated(0, 0, normed(cring[slot, rows, :].astype(F32)), hbuf[slot, rows, :].astype(F32))
        row_blocks(rows_body)
        remote(out.at[s], out.at[s], sx0, rx0.at[n], dev_c).start()
        @pl.when(n + 2 * own < steps)
        def _():
            load_sample(n + 2 * own)

    def qb_rows(off, n):
        return qb0[pl.ds(off, n), :]

    ada_cps[0].wait()
    load_attn(0, lambda off, n: qb0.at[pl.ds(off, n)], s_loc.at[0])
    for n in range(1, 2 * own):
        load_sample(n)
    load_attn(1, own_rows(1), s_loc.at[2])
    load_rest(1, own_rows(1), s_loc.at[2])
    for cp in (cond_cp, act_cp, zero_cps[0], *ada_cps[1:], *zero_cps[1:]):
        cp.start()
    pl.semaphore_wait(barrier, len(devs))
    wait_like(buf.at[x, pl.ds(0, g.lr - g.o0)], s_loc.at[1])
    early = (g.lr - g.o0) // CH
    for k in range(min(LA, early)):
        first(k)
    ada_first(0)
    wait_like(qb0, s_loc.at[0])
    bias_prep(qb_rows)
    for d in (dev_p, dev_m, dev_o):
        remote(bqbuf.at[x], bqbuf.at[x], s_bq, r_bq, d).start()
    q_bias0 = bqbuf[x, pl.ds(0, 1), :]
    project(slot_a, out[sample_of(0, c)], qb_rows, q_bias0)
    wait_like(buf.at[x, pl.ds(0, g.lr)], s_loc.at[2])
    for k in range(min(LA, early), LA):
        first(k)

    def first_steps(m, carry):
        @pl.when(m + 1 < steps)
        def _():
            ada_first(m + 1)

        def slot_of(pair, core):
            return jnp.where(pair == c, 0, own) + core

        def place_of(u, core):
            slot = slot_of(pair_of(m), core) * nx + x
            return slot, jnp.where(m < steps - own, stage0 + CORES * m + u, slot)

        def send(u, slot, place):
            @pl.when(m == 0)
            def _():
                remote(obuf.at[place], relay_box(u), s_o, r_rel.at[u], dev_p).start()

            @pl.when(m == 1)
            def _():
                remote(obuf.at[place], relay_box(CORES + u), s_o, r_rel.at[CORES + u], dev_m).start()

            @pl.when((m >= own) & (m < steps - own))
            def _():
                remote(obuf.at[place], obuf.at[slot], s_o, r_o, {'tp': chip_of(m) * CORES + c}).start()

        def forward(pair, dev, source):
            for u, core in enumerate((c, 1 - c)):
                r = relay_box(pair * CORES + u)
                wait_like(r, r_rel.at[pair * CORES + u])
                remote(r, obuf.at[slot_of(pair, core) * nx + source], s_o, r_o, dev).start()

        @pl.when(m == own)
        def _():
            forward(0, dev_p, xm)

        @pl.when(m == own + 1)
        def _():
            forward(1, dev_m, xp)
        wait_like(out.at[0], rx0.at[m])
        slot, place = place_of(0, c)
        attend(slot_a, obuf.at[place])
        project(slot_b, out[sample_of(m, 1 - c)], qb_rows, q_bias0)
        send(0, slot, place)
        slot, place = place_of(1, 1 - c)
        attend(slot_b, obuf.at[place])
        project(slot_a, out[sample_of(jnp.minimum(m + 1, steps - 1), c)], qb_rows, q_bias0)
        send(1, slot, place)

        @pl.when(m >= HELD)
        def _():
            tick(m - HELD)
        return carry
    lax.fori_loop(0, steps, first_steps, 0)

    cond_cp.wait()
    act_cp.wait()
    for i in range(own):
        lnbuf[i] = normed(cbuf[i].astype(F32))
    for cp in (*ada_cps[1:], *zero_cps):
        cp.wait()
    remote_pieces = CORES * (steps - own)
    wait_like(obuf.at[pl.ds(stage0, remote_pieces)], r_o)
    wait_like(obuf.at[pl.ds(0, remote_pieces + CORES * own)], s_o)
    wait_like(out.at[pl.ds(0, steps)], sx0)

    def attn_part(l, i, rows):
        lhs = jnp.concatenate([obuf[i * nx + s, rows, :] for s in range(nx)], axis=1)
        zpad = jnp.zeros((LANES - lw, LANES), BF16)
        rhs = jnp.concatenate([jnp.concatenate([v for s in range(nx) for v in (flat(s, l, g.o0 + j * lw, lw), zpad)], axis=0) for j in range(g.ncol)], axis=1)
        return dot_nn(lhs, rhs)

    def up_sample(l, i):
        y = xbuf[i]
        for p in range(nx // 2):
            w = jnp.concatenate([jnp.concatenate([flat(2 * p + e, l, g.u0 + j * 2 * hu, 2 * hu) for j in range(g.ncol)], axis=1) for e in range(2)], axis=0)
            u = dot_nt(y, w)
            mids = []
            for e in range(2):
                ua, ub, uc = (u[:, (3 * e + v) * LANES:(3 * e + v + 1) * LANES] for v in range(3))
                side = (3 * p + 2 * e) * LANES
                hbuf[i, :, side:side + LANES] = (jax.nn.silu(ua) * uc).astype(BF16)
                act = jax.nn.silu(ub)
                mids.append(act * pltpu.roll(ub, half, 1) if e == 0 else pltpu.roll(act, half, 1) * ub)
            mid = (3 * p + 1) * LANES
            hbuf[i, :, mid:mid + LANES] = jnp.where(lane < half, mids[0], mids[1]).astype(BF16)

    def trans_part(l, i, rows):
        cols = []
        for j in range(g.ncol):
            v = []
            for p in range(nx // 2):
                v.append(flat(2 * p, l, g.d0 + j * hu, hu))
                v.append(flat(2 * p + 1, l, g.d0 + j * hu + LANES, half))
                v.append(flat(2 * p + 1, l, g.d0 + j * hu, LANES))
            cols.append(jnp.concatenate(v, axis=0))
        return dot_nn(hbuf[i, rows, :], jnp.concatenate(cols, axis=1))

    PR = OUT_ROWS
    npc = T // PR
    tpp, tpm, tpo = (v * CORES + c for v in (xp, xm, xo))

    def orow(blk, p, lo=0, n=PR):
        return out.at[blk * own + p // npc, pl.ds(pl.multiple_of(lax.rem(p, npc) * PR, PR) + lo, n)]

    def opush(r, dev, sem):
        remote(r, r, osend, sem, dev).start()

    def oawait(halves, sem):
        wait_like(out.at[0, pl.ds(0, halves * PR // 2)], sem)

    def out_first(i):
        for h in range(npc):
            p = i * npc + h
            opush(orow(tp, p), dev_p, o_a.at[p])
            opush(orow(tp, p), dev_m, o_a.at[p])
            opush(orow(tp, p), dev_c, o_p0.at[p])

    def out_relay(p):
        oawait(4, o_a.at[p])
        opush(orow(tpm, p, 0, PR // 2), dev_p, o_d.at[p])
        opush(orow(tpp, p, PR // 2, PR // 2), dev_m, o_d.at[p])
        opush(orow(tpm, p), dev_c, o_p1.at[p])
        opush(orow(tpp, p), dev_c, o_p1.at[p])

    t0 = steps - HELD
    t1 = t0 + TAIL_TICKS
    assert K + LAGS[-1] <= t1 + nx * own and need(g.lr, LAGS[-1]) <= t0 + 4

    def arrived(lo, hi):
        for k in range(lo, hi):
            stage4(k)

    k_o, k_u, k_d = (need(v, 0) for v in (g.u0, g.d0, g.lr))
    def each(count):
        def run(body):
            def step(i, carry):
                body(i)
                return carry
            lax.fori_loop(0, count, step, 0)
        return run

    arrived(0, k_o)

    @each(own)
    def _(i):
        part_sample(0, i, attn_part)
    tick(t0)

    @each(own)
    def _(i):
        resid_sample(0, 0, i, attn_part)
        ada_sample(0, 1, i)
        tick(t0 + 1 + i)
    arrived(k_o, k_u)

    @each(2 * own)
    def _(i):
        @pl.when(i >= own)
        def _():
            wait_like(xbuf.at[0], rx.at[i - own])
        up_sample(0, i)

        @pl.when(lax.rem(i, 2) == 1)
        def _():
            tick(t0 + 3 + i // 2)
    arrived(k_u, k_d)

    @each(own)
    def _(i):
        wait_like(sent_part(0), sp.at[i])
        part_sample(0, i, trans_part)
        wait_like(xbuf.at[0], sx.at[i])

    @each(own)
    def _(i):
        resid_sample(0, 1, i, trans_part)
        ada_sample(1, 0, i)
        tick(t0 + 5 + i)
    wait_like(bqbuf.at[pl.ds(0, nx - 1)], r_bq)

    k_q, k_o, k_u, k_d = (need(g.lr + v, 0) for v in (g.o0, g.u0, g.d0, g.lr))
    first_k = need(g.lr, 0)

    def shard_of(q):
        return lax.rem(x + jnp.where(q == 0, 0, jnp.where(q == 1, nx - 1, q - 1)), nx)

    def rows_from(s):
        return lambda off, n: flat(s, 1, off, n)

    def q_bias1(s):
        return bqbuf[s, pl.ds(1, 1), :]

    def half_layer(hf, carry):
        def once(body):
            pl.when(hf == 0)(body)

        project(slot_a, xbuf[hf], rows_from(x), q_bias1(x))
        wait_like(xbuf.at[own + hf], rx.at[hf])

        def shard(q, inner):
            s = shard_of(q)
            after = shard_of(jnp.minimum(q + 1, nx - 1))
            bias_prep(rows_from(s))
            pl.when((hf > 0) & (q == RELAY_AT))(lambda: out_relay(0))
            attend(slot_a, obuf.at[hf * nx + s])
            project(slot_b, xbuf[own + hf], rows_from(s), q_bias1(s))

            @pl.when(hf == 0)
            def _():
                tick(t1 + 2 * q)

                @pl.when(q == nx - 2)
                def _():
                    arrived(first_k, k_q)
            attend(slot_b, obuf.at[(own + hf) * nx + s])
            project(slot_a, xbuf[hf], rows_from(after), q_bias1(after))
            once(lambda: tick(t1 + 2 * q + 1))
            return inner
        lax.fori_loop(0, nx, shard, 0)
        once(lambda: arrived(k_q, k_o))
        wait_like(sent_part(hf), sp.at[hf])
        part_sample(1, hf, attn_part)
        wait_like(xbuf.at[hf], sx.at[hf])
        resid_sample(1, 0, hf, attn_part)
        ada_sample(1, 1, hf)
        once(lambda: arrived(k_o, k_u))
        pl.when(hf > 0)(lambda: out_relay(1))
        up_sample(1, hf)
        wait_like(xbuf.at[own + hf], rx.at[hf])
        up_sample(1, own + hf)
        once(lambda: arrived(k_u, k_d))
        wait_like(sent_part(hf), sp.at[hf])
        part_sample(1, hf, trans_part)
        resid_sample(1, 1, hf, trans_part)
        out_first(hf)
        return carry

    lax.fori_loop(0, own, half_layer, 0)
    for i in range(own):
        wait_like(xbuf.at[i], sx.at[i])
        wait_like(sent_part(i), sp.at[i])
    for p in range(npc, own * npc):
        out_relay(p)
    for p in range(own * npc):
        oawait(2, o_d.at[p])
        opush(orow(tpo, p), dev_c, o_p2.at[p])
    for p in range(own * npc):
        oawait(2, o_p0.at[p])
        oawait(4, o_p1.at[p])
        oawait(2, o_p2.at[p])
    wait_like(out.at[pl.ds(0, 7 * own)], osend)
    wait_like(buf.at[pl.ds(0, 3)], send)
    wait_like(bqbuf.at[pl.ds(0, nx - 1)], s_bq)


def finish(src, dst, sem):
    cp = pltpu.make_async_copy(src, dst, sem)
    cp.start()
    cp.wait()


def solution(mesh):
    def body(token_act, token_cond, pair_bias, token_mask, ada_scale, ada_w, ada_bias, zero_w, zero_b, w_qkvg, b_q, w_o, w_up, w_down):
        g = Geometry(mesh, token_act.shape, token_cond.shape, pair_bias.shape, w_qkvg.shape, w_up.shape)
        L, D, C, T, own, nx = g.layers, g.width, g.cond_dim, g.tokens, g.own, g.nx
        ada = ada_w.transpose(0, 1, 3, 2, 4).reshape(2 * L, 2, C, D)
        zero = zero_w.transpose(0, 2, 1, 3).reshape(2 * L, C, D)
        vm = pl.BlockSpec(memory_space=pltpu.VMEM)
        hbm = pl.BlockSpec(memory_space=pl.ANY)
        dma = pltpu.SemaphoreType.DMA
        npc = own * (T // OUT_ROWS)
        K = g.chunks
        steps = nx * own
        gathered = pl.pallas_call(
            functools.partial(kernel, g),
            out_shape=pltpu.VMEM(token_act.shape, BF16),
            in_specs=[hbm, hbm, hbm, vm, vm, hbm, vm, hbm, vm, hbm, vm, hbm, hbm, hbm],
            out_specs=vm,
            scratch_shapes=[
                pltpu.VMEM((nx, g.rows, LANES), BF16),
                pltpu.VMEM((g.o0, LANES), BF16),
                pltpu.VMEM((2 * own, T, D), BF16),
                pltpu.VMEM((own, T, D), BF16),
                pltpu.VMEM((own * g.ncol, T, LANES), BF16),
                pltpu.VMEM((2 * own * nx + own * g.ncol, T, LANES), BF16),
                pltpu.VMEM((2 * own, T, nx * g.hu), BF16),
                pltpu.VMEM((2 * own, T, C), BF16),
                pltpu.VMEM((own, T, C), BF16),
                pltpu.VMEM((own, T, C), F32),
                pltpu.VMEM((2 * L, 2, C, D), BF16),
                pltpu.VMEM((2 * L, C, D), BF16),
                pltpu.VMEM((nx, 8, LANES), F32),
                pltpu.VMEM((g.heads, T, T), F32),
                pltpu.VMEM((T, LANES), BF16),
                pltpu.VMEM((T, LANES), BF16),
                pltpu.VMEM((T, LANES), BF16),
                pltpu.VMEM((T, LANES), F32),
                pltpu.VMEM((T, LANES), BF16),
                pltpu.VMEM((T, LANES), BF16),
                pltpu.VMEM((T, LANES), BF16),
                pltpu.VMEM((T, LANES), F32),
                dma((3,)), dma((3,)), dma((4 * L,)), dma((2, 2 * own)), dma,
                dma((K,)), dma((K,)), dma((K,)), dma((K,)),
                dma, dma, dma, dma((steps,)), dma, dma, dma((CORES * own,)),
                dma((own,)), dma((own,)), dma((own,)), dma((own,)),
                dma, dma((npc,)), dma((npc,)), dma((npc,)), dma((npc,)), dma((npc,)),
            ],
            compiler_params=pltpu.CompilerParams(collective_id=0, has_side_effects=True, vmem_limit_bytes=207 << 18),
            name='blocks',
        )(token_act, token_cond, pair_bias, token_mask.reshape(1, T), ada_scale, ada, ada_bias, zero, zero_b, w_qkvg.transpose(0, 2, 3, 1), b_q, w_o, w_up.transpose(0, 2, 3, 1), w_down)
        gathered = pltpu.with_memory_space_constraint(gathered, pltpu.VMEM)
        return pl.pallas_call(
            finish,
            out_shape=jax.ShapeDtypeStruct(token_act.shape, BF16),
            in_specs=[vm],
            out_specs=pl.BlockSpec(memory_space=pltpu.HBM),
            scratch_shapes=[dma],
            compiler_params=pltpu.CompilerParams(vmem_limit_bytes=1 << 20),
            name='finish',
        )(gathered)

    everywhere = P()
    in_specs = (P('dp', None, None), P('dp', None, None), P(None, 'tp', None, None), P(None), everywhere, everywhere, everywhere, everywhere, everywhere, P(None, None, None, 'tp'), P(None, 'tp'), P(None, 'tp', None), P(None, None, None, 'tp'), P(None, 'tp', None))
    return jax.shard_map(body, mesh=mesh, in_specs=in_specs, out_specs=P('dp', None, None), check_vma=False)
```

```python
import functools
import math
import jax
import jax.numpy as jnp
from jax import lax
from jax.experimental import pallas as pl
from jax.experimental.pallas import tpu as pltpu
from jax.sharding import PartitionSpec as P

LN_EPS = 1e-5
LOG2E = 1.4426950408889634
MESH = pl.DeviceIdType.MESH
BF16 = jnp.bfloat16
F32 = jnp.float32
LANES = 128
CH = 1216
LA = 4
TAIL_TICKS = 6
HELD = 0
LAGS = (0, 2, 5)
RB = 512
OUT_ROWS = 256
CORES = 2


def dot_nt(lhs, rhs):
    return lax.dot_general(lhs, rhs, (((1,), (1,)), ((), ())), preferred_element_type=F32)


def dot_nn(lhs, rhs):
    return lax.dot_general(lhs, rhs, (((1,), (0,)), ((), ())), preferred_element_type=F32)


def normed(values_in):
    row_mean = jnp.mean(values_in, axis=-1, keepdims=True)
    centered = values_in - row_mean
    variance = jnp.mean(centered * centered, axis=-1, keepdims=True)
    return centered * lax.rsqrt(variance + LN_EPS)


class Geometry:
    def __init__(self, mesh, act, cond, bias, w_qkvg, w_up):
        self.nx = mesh.shape['tp'] // CORES
        self.y_stride = len({d.coords[2] for d in mesh.devices.flat})
        self.samples, self.tokens, self.width = act
        self.cond_dim = cond[-1]
        self.layers, self.heads = bias[0], bias[1]
        self.lw = w_qkvg[-1]
        self.hd = self.lw // self.heads
        self.hu = w_up[-1]
        self.own = self.samples // mesh.shape['tp']
        self.ncol = self.width // LANES
        self.tcol = self.tokens // LANES
        self.q0 = 0
        self.b0 = self.q0 + self.ncol * 4 * self.lw
        self.o0 = self.b0 + self.heads * self.tcol * self.tokens
        self.u0 = self.o0 + self.ncol * self.lw
        self.d0 = self.u0 + self.ncol * 2 * self.hu
        self.lr = self.d0 + self.ncol * self.hu
        self.flat_rows = self.layers * self.lr - self.o0
        self.chunks = -(-self.flat_rows // CH)
        self.rows = self.chunks * CH
        assert self.lw == 96 and self.hu == 192 and self.heads == 2 and self.nx == 4 and self.layers == 2 and self.own == 2


def kernel(g, act_in, cond_in, bias_in, mask_in, ascale_in, ada_in, abias_in, zero_in, zbias_in, wq_in, bq_in, wo_in, up_in, down_in,
           out, buf, qb0, xbuf, abuf, pbuf, sbuf, obuf, hbuf, cring, cbuf, lnbuf, adabuf, zerobuf, bqbuf, mcol, bmbuf, qa, ka, va, ga, qb, kb, vb, gb,
           s_loc, s_act, s_bias, s_ada, s_in, send, ra, rb, rc, rd, s_bq, r_bq, sx0, rx0, s_o, r_o, r_rel, sx, rx, sp, rp, osend, o_p0, o_a, o_p1, o_d, o_p2):
    nx, own, T, D = g.nx, g.own, g.tokens, g.width
    lw, hu, hd = g.lw, g.hu, g.hd
    half = hu - LANES
    tp = lax.axis_index('tp')
    dp = lax.axis_index('dp')
    x = tp // CORES
    c = lax.rem(tp, CORES)
    xp = lax.rem(x + 1, nx)
    xm = lax.rem(x + nx - 1, nx)
    xo = lax.rem(x + 2, nx)
    dev_p, dev_m, dev_o = ({'tp': v * CORES + c} for v in (xp, xm, xo))
    dev_c = {'tp': x * CORES + 1 - c}
    pz = lax.rem(dp, 2)
    py = lax.rem(dp // g.y_stride, 2)
    dev_z = {'dp': dp + 1 - 2 * pz}
    dev_y = {'dp': dp + g.y_stride * (1 - 2 * py)}
    mine = tp * own

    def remote(src, dst, s_sem, r_sem, dev):
        return pltpu.make_async_remote_copy(src, dst, s_sem, r_sem, device_id=dev, device_id_type=MESH)

    def wait_like(ref, sem):
        pltpu.make_async_copy(ref, ref, sem).wait()

    barrier = pltpu.get_barrier_semaphore()
    devs = (dev_p, dev_m, dev_o, dev_c, dev_z, dev_y)
    for d in devs:
        pl.semaphore_signal(barrier, inc=1, device_id=d, device_id_type=MESH)

    steps = nx * own

    def chip_of(n):
        near = jnp.where(lax.rem(n, 2) == 0, 1, nx - 1)
        return lax.rem(x + jnp.where(n < own, 2, jnp.where(n < 3 * own, near, 0)), nx)

    def pair_of(n):
        return jnp.where((n < own) | (n >= 3 * own), lax.rem(n, own), (n - own) // 2)

    def sample_of(n, core):
        return chip_of(n) * (CORES * own) + pair_of(n) * CORES + core

    def load_sample(n):
        slot = lax.rem(n, 2 * own)
        pltpu.make_async_copy(act_in.at[sample_of(n, c)], hbuf.at[slot], s_in.at[0, slot]).start()
        pltpu.make_async_copy(cond_in.at[sample_of(n, c)], cring.at[slot], s_in.at[1, slot]).start()

    load_sample(0)
    ada_cps = [pltpu.make_async_copy(ada_in.at[v], adabuf.at[v], s_ada.at[v]) for v in range(2 * g.layers)]
    zero_cps = [pltpu.make_async_copy(zero_in.at[v], zerobuf.at[v], s_ada.at[2 * g.layers + v]) for v in range(2 * g.layers)]
    ada_cps[0].start()

    u_parts = ((0, 0, LANES, 0), (0, LANES, half, LANES), (1, LANES, half, LANES + half), (1, 0, LANES, 2 * LANES))

    def load_attn(l, place, sem):
        for j in range(g.ncol):
            for f in range(4):
                pltpu.make_async_copy(wq_in.at[l, f, :, pl.ds(j * LANES, LANES)], place(g.q0 + (j * 4 + f) * lw, lw), sem).start()

    def load_bias(l):
        for h in range(g.heads):
            pltpu.make_async_copy(bias_in.at[l, h], abuf.at[h, :, pl.ds(0, T)], s_bias).start()

    def turn_bias(l, put):
        for h in range(g.heads):
            wait_like(abuf.at[h, :, pl.ds(0, T)], s_bias)
        for h in range(g.heads):
            for j in range(g.tcol):
                put(g.b0 + (h * g.tcol + j) * T, abuf[h, pl.ds(j * LANES, LANES), pl.ds(0, T)].T)

    def load_rest(l, place, sem):
        for j in range(g.ncol):
            col = pl.ds(j * LANES, LANES)
            pltpu.make_async_copy(wo_in.at[l, :, col], place(g.o0 + j * lw, lw), sem).start()
            for f, r0, n, off in u_parts:
                pltpu.make_async_copy(up_in.at[l, f, pl.ds(r0, n), col], place(g.u0 + j * 2 * hu + off, n), sem).start()
            pltpu.make_async_copy(down_in.at[l, :, col], place(g.d0 + j * hu, hu), sem).start()

    def own_rows(l):
        return lambda off, n: buf.at[x, pl.ds(l * g.lr - g.o0 + off, n)]

    load_bias(0)
    load_rest(0, own_rows(0), s_loc.at[1])
    act_cp = pltpu.make_async_copy(act_in.at[pl.ds(mine, own)], abuf, s_act.at[0])
    cond_cp = pltpu.make_async_copy(cond_in.at[pl.ds(mine, own)], cbuf, s_act.at[1])
    bqbuf[x] = jnp.zeros((8, LANES), F32)
    bqbuf[x, pl.ds(0, g.layers), pl.ds(0, lw)] = bq_in[...]

    pad = g.rows - g.flat_rows
    if pad:
        buf[x, pl.ds(g.flat_rows, pad), :] = jnp.zeros((pad, LANES), BF16)

    Q = CH // 4
    g0 = 2 * py + pz
    gy = 2 * (1 - py) + pz
    gz = 2 * py + 1 - pz
    gd = 2 * (1 - py) + 1 - pz

    def push(blk, k, part, dev, r_sem):
        r = buf.at[blk, pl.ds(pl.multiple_of(k * CH + part * Q, 8), Q)]
        remote(r, r, send, r_sem, dev).start()

    def await_quarters(n, sem):
        wait_like(buf.at[0, pl.ds(0, n * Q)], sem)

    def first(k):
        push(x, k, g0, dev_p, ra.at[k])
        push(x, k, g0, dev_m, ra.at[k])

    def stage1(k):
        await_quarters(2, ra.at[k])
        for blk in (xm, xp):
            push(blk, k, g0, dev_y, rb.at[k])
            push(blk, k, g0, dev_z, rb.at[k])

    def stage2(k):
        await_quarters(4, rb.at[k])
        push(xm, k, gz, dev_y, rc.at[k])
        push(xp, k, gy, dev_z, rc.at[k])

    def stage3(k):
        await_quarters(2, rc.at[k])
        for part in (g0, gy):
            push(xm, k, part, dev_p, rd.at[k])
        for part in (gz, gd):
            push(xp, k, part, dev_m, rd.at[k])

    def stage4(k):
        await_quarters(4, rd.at[k])

    K = g.chunks

    def tick(t):
        @pl.when(t + LA < K)
        def _():
            first(t + LA)
        for lag, stage in zip(LAGS, (stage1, stage2, stage3)):
            @pl.when((t >= lag) & (t - lag < K))
            def _(lag=lag, stage=stage):
                stage(t - lag)

    def need(rows_end, lag):
        return -(-(rows_end - g.o0) // CH) + lag

    lane = lax.broadcasted_iota(jnp.int32, (1, LANES), 1)
    scale2 = LOG2E / math.sqrt(hd)

    def modulated(l, j, cond_ln, act_of):
        c_in = (cond_ln * ascale_in[l, pl.ds(j, 1), :]).astype(BF16)
        gain = dot_nn(c_in, adabuf[l * 2 + j, 0])
        shift = dot_nn(c_in, adabuf[l * 2 + j, 1])
        act_ln = normed(act_of().astype(F32))
        return (jax.nn.sigmoid(gain + abias_in[l, pl.ds(j, 1), :]) * act_ln + shift).astype(BF16)

    def row_blocks(body):
        for r in range(T // RB):
            body(pl.ds(r * RB, RB))

    def ada_sample(l, j, i):
        def rows_body(rows):
            xbuf[i, rows, :] = modulated(l, j, lnbuf[i, rows, :], lambda: abuf[i, rows, :])
        row_blocks(rows_body)
        remote(xbuf.at[i], xbuf.at[own + i], sx.at[i], rx.at[i], dev_c).start()

    stage0 = 2 * own * nx

    def relay_box(v):
        return xbuf.at[v, pl.ds(0, lw), pl.ds(0, T)]

    def resid_sample(l, j, i, part_of):
        rows = pl.ds(0, T)
        ours = part_of(l, i, rows)
        gate = jax.nn.sigmoid(dot_nn(cbuf[i], zerobuf[l * 2 + j]) + zbias_in[l, pl.ds(j, 1), :])
        wait_like(pbuf.at[i], rp.at[i])
        act = (abuf[i].astype(F32) + gate * (ours + pbuf[i].astype(F32)).astype(BF16).astype(F32)).astype(BF16)
        abuf[i] = act
        if j == 1:
            out[mine + i] = act

    def part_sample(l, i, part_of):
        sbuf[i] = part_of(l, own + i, pl.ds(0, T)).astype(BF16)
        remote(sbuf.at[i], pbuf.at[i], sp.at[i], rp.at[i], dev_c).start()

    def flat(s, l, off, n):
        return buf[s, pl.ds(pl.multiple_of(l * g.lr - g.o0 + off, 8), n), :]

    def bias_prep(rows_of):
        for h in range(g.heads):
            for j in range(g.tcol):
                col = pl.ds(j * LANES, LANES)
                bmbuf[h, :, col] = rows_of(g.b0 + (h * g.tcol + j) * T, T).astype(F32) * LOG2E + mcol[...]

    def project_dot(x_rows, rows_of):
        w = jnp.concatenate([rows_of(g.q0 + j * 4 * lw, 4 * lw) for j in range(g.ncol)], axis=1)
        return dot_nt(w, x_rows)

    def project_end(slot, proj, q_bias):
        qs, ks, vs, gs = slot
        qs[...] = (proj[:lw] + q_bias).astype(BF16)
        ks[...] = proj[lw:2 * lw].astype(BF16).T
        vs[...] = proj[2 * lw:3 * lw].astype(BF16)
        gs[...] = jax.nn.sigmoid(proj[3 * lw:])

    def scores(slot, h):
        qs, ks, _, _ = slot
        none = jnp.zeros((hd, T), BF16)
        q = jnp.concatenate([qs[pl.ds(h * hd, hd), :] if v == h else none for v in range(g.heads)], axis=0)
        return dot_nn(ks[...], q)

    def weights(h, s):
        z = s * scale2 + bmbuf[h]
        return jnp.exp2(z - jnp.max(z, axis=0, keepdims=True)).astype(BF16)

    def mix(slot, h, e, o_ref):
        _, _, vs, gs = slot
        mine_h = pl.ds(h * hd, hd)
        o = dot_nn(jnp.concatenate([vs[mine_h, :], jnp.ones((16, T), BF16)], axis=0), e)
        o_ref[mine_h, :] = (o[:hd] * (1.0 / o[hd:hd + 1]) * gs[mine_h, :]).astype(BF16)

    def project(slot, x_rows, rows_of, q_bias):
        project_end(slot, project_dot(x_rows, rows_of), q_bias)

    def pair(slot, o_ref, after, x_rows, rows_of, q_bias):
        s0 = scores(slot, 0)
        s1 = scores(slot, 1)
        proj = project_dot(x_rows, rows_of)
        e0 = weights(0, s0)
        mix(slot, 0, e0, o_ref)
        e1 = weights(1, s1)
        mix(slot, 1, e1, o_ref)
        project_end(after, proj, q_bias)
    slot_a = (qa, ka, va, ga)
    slot_b = (qb, kb, vb, gb)

    def ada_first(n):
        slot = lax.rem(n, 2 * own)
        s = sample_of(n, c)
        wait_like(hbuf.at[slot], s_in.at[0, slot])
        wait_like(cring.at[slot], s_in.at[1, slot])
        def rows_body(rows):
            out[s, rows, :] = modulated(0, 0, normed(cring[slot, rows, :].astype(F32)), lambda: hbuf[slot, rows, :])
        row_blocks(rows_body)
        remote(out.at[s], out.at[s], sx0, rx0.at[n], dev_c).start()
        @pl.when(n + 2 * own < steps)
        def _():
            load_sample(n + 2 * own)

    def qb_rows(off, n):
        return qb0[pl.ds(off, n), :]

    ada_cps[0].wait()
    load_attn(0, lambda off, n: qb0.at[pl.ds(off, n)], s_loc.at[0])
    for n in range(1, 2 * own):
        load_sample(n)
    load_attn(1, own_rows(1), s_loc.at[2])
    load_rest(1, own_rows(1), s_loc.at[2])
    for cp in (cond_cp, zero_cps[0], *ada_cps[1:], *zero_cps[1:]):
        cp.start()
    pl.semaphore_wait(barrier, len(devs))
    wait_like(buf.at[x, pl.ds(0, g.lr - g.o0)], s_loc.at[1])
    early = (g.lr - g.o0) // CH
    for k in range(min(LA, early)):
        first(k)
    ada_first(0)
    mask_col = jnp.broadcast_to((mask_in[...].astype(F32) - 1.0) * (1e9 * LOG2E), (8, T)).T
    mcol[...] = jnp.broadcast_to(mask_col[:, 0:1], (T, LANES))

    def put_first(off, v):
        qb0[pl.ds(off, T), :] = v
    turn_bias(0, put_first)
    load_bias(1)
    wait_like(qb0.at[pl.ds(0, g.b0)], s_loc.at[0])
    bias_prep(qb_rows)
    for d in (dev_p, dev_m, dev_o):
        remote(bqbuf.at[x], bqbuf.at[x], s_bq, r_bq, d).start()
    q_bias0 = bqbuf[x].T[:lw, 0:1]
    project(slot_a, out[sample_of(0, c)], qb_rows, q_bias0)
    wait_like(buf.at[x, pl.ds(0, g.lr - g.o0 + g.b0)], s_loc.at[2])
    for k in range(min(LA, early), LA):
        first(k)

    def put_second(off, v):
        buf[x, pl.ds(g.lr - g.o0 + off, T), :] = v

    def first_steps(m, carry):
        @pl.when(m == 1)
        def _():
            turn_bias(1, put_second)
            act_cp.start()

        @pl.when(m + 1 < steps)
        def _():
            ada_first(m + 1)

        def slot_of(pair, core):
            return jnp.where(pair == c, 0, own) + core

        def place_of(u, core):
            slot = slot_of(pair_of(m), core) * nx + x
            return slot, jnp.where(m < steps - own, stage0 + CORES * m + u, slot)

        def send(u, slot, place):
            @pl.when(m == 0)
            def _():
                remote(obuf.at[place], relay_box(u), s_o, r_rel.at[u], dev_p).start()

            @pl.when(m == 1)
            def _():
                remote(obuf.at[place], relay_box(CORES + u), s_o, r_rel.at[CORES + u], dev_m).start()

            @pl.when((m >= own) & (m < steps - own))
            def _():
                remote(obuf.at[place], obuf.at[slot], s_o, r_o, {'tp': chip_of(m) * CORES + c}).start()

        def forward(pair, dev, source):
            for u, core in enumerate((c, 1 - c)):
                r = relay_box(pair * CORES + u)
                wait_like(r, r_rel.at[pair * CORES + u])
                remote(r, obuf.at[slot_of(pair, core) * nx + source], s_o, r_o, dev).start()

        @pl.when(m == own + 1)
        def _():
            forward(0, dev_p, xm)

        @pl.when(m == own + 2)
        def _():
            forward(1, dev_m, xp)
        wait_like(out.at[0], rx0.at[m])
        slot, place = place_of(0, c)
        pair(slot_a, obuf.at[place], slot_b, out[sample_of(m, 1 - c)], qb_rows, q_bias0)
        send(0, slot, place)
        slot, place = place_of(1, 1 - c)
        pair(slot_b, obuf.at[place], slot_a, out[sample_of(jnp.minimum(m + 1, steps - 1), c)], qb_rows, q_bias0)
        send(1, slot, place)

        @pl.when(m >= HELD)
        def _():
            tick(m - HELD)
        return carry
    lax.fori_loop(0, steps, first_steps, 0)

    cond_cp.wait()
    act_cp.wait()
    for i in range(own):
        lnbuf[i] = normed(cbuf[i].astype(F32))
    for cp in (*ada_cps[1:], *zero_cps):
        cp.wait()
    remote_pieces = CORES * (steps - own)
    wait_like(obuf.at[pl.ds(stage0, remote_pieces)], r_o)
    wait_like(obuf.at[pl.ds(0, remote_pieces + CORES * own)], s_o)
    wait_like(out.at[pl.ds(0, steps)], sx0)

    def attn_part(l, i, rows):
        lhs = jnp.concatenate([obuf[i * nx + s] for s in range(nx)], axis=0)
        rhs = jnp.concatenate([jnp.concatenate([flat(s, l, g.o0 + j * lw, lw) for s in range(nx)], axis=0) for j in range(g.ncol)], axis=1)
        return lax.dot_general(lhs, rhs, (((0,), (0,)), ((), ())), preferred_element_type=F32)

    def up_sample(l, i):
        y = xbuf[i]
        pre = []
        for p in range(nx // 2):
            w = jnp.concatenate([jnp.concatenate([flat(2 * p + e, l, g.u0 + j * 2 * hu, 2 * hu) for j in range(g.ncol)], axis=1) for e in range(2)], axis=0)
            pre.append(dot_nt(y, w))
        for p in range(nx // 2):
            mids = []
            for e in range(2):
                ua, ub, uc = (pre[p][:, (3 * e + v) * LANES:(3 * e + v + 1) * LANES] for v in range(3))
                side = (3 * p + 2 * e) * LANES
                hbuf[i, :, side:side + LANES] = (jax.nn.silu(ua) * uc).astype(BF16)
                act = jax.nn.silu(ub)
                mids.append(act * pltpu.roll(ub, half, 1) if e == 0 else pltpu.roll(act, half, 1) * ub)
            mid = (3 * p + 1) * LANES
            hbuf[i, :, mid:mid + LANES] = jnp.where(lane < half, mids[0], mids[1]).astype(BF16)

    def trans_part(l, i, rows):
        cols = []
        for j in range(g.ncol):
            v = []
            for p in range(nx // 2):
                v.append(flat(2 * p, l, g.d0 + j * hu, hu))
                v.append(flat(2 * p + 1, l, g.d0 + j * hu + LANES, half))
                v.append(flat(2 * p + 1, l, g.d0 + j * hu, LANES))
            cols.append(jnp.concatenate(v, axis=0))
        return dot_nn(hbuf[i, rows, :], jnp.concatenate(cols, axis=1))

    PR = OUT_ROWS
    npc = T // PR
    tpp, tpm, tpo = (v * CORES + c for v in (xp, xm, xo))

    def orow(blk, p, lo=0, n=PR):
        return out.at[blk * own + p // npc, pl.ds(pl.multiple_of(lax.rem(p, npc) * PR, PR) + lo, n)]

    def opush(r, dev, sem):
        remote(r, r, osend, sem, dev).start()

    def oawait(halves, sem):
        wait_like(out.at[0, pl.ds(0, halves * PR // 2)], sem)

    def out_first(i):
        for h in range(npc):
            p = i * npc + h
            opush(orow(tp, p), dev_p, o_a.at[p])
            opush(orow(tp, p), dev_m, o_a.at[p])
            opush(orow(tp, p), dev_c, o_p0.at[p])

    def out_relay(p):
        oawait(4, o_a.at[p])
        opush(orow(tpm, p, 0, PR // 2), dev_p, o_d.at[p])
        opush(orow(tpp, p, PR // 2, PR // 2), dev_m, o_d.at[p])
        opush(orow(tpm, p), dev_c, o_p1.at[p])
        opush(orow(tpp, p), dev_c, o_p1.at[p])

    t0 = steps - HELD
    t1 = t0 + TAIL_TICKS
    assert K + LAGS[-1] <= t1 + nx and need(g.d0, LAGS[-1]) <= t0 + 2 and need(g.lr, LAGS[-1]) <= t0 + 4
    assert need(g.lr + g.o0, LAGS[-1]) <= t1 + nx - 1 and need(g.lr + g.o0, LAGS[2]) <= t1

    def arrived(lo, hi):
        for k in range(lo, hi):
            stage4(k)

    k_o, k_u, k_d = (need(v, 0) for v in (g.u0, g.d0, g.lr))
    def each(count):
        def run(body):
            def step(i, carry):
                body(i)
                return carry
            lax.fori_loop(0, count, step, 0)
        return run

    arrived(0, k_o)

    @each(own)
    def _(i):
        part_sample(0, i, attn_part)

    @each(own)
    def _(i):
        resid_sample(0, 0, i, attn_part)
        ada_sample(0, 1, i)
        tick(t0 + i)
    arrived(k_o, k_u)

    @each(2 * own)
    def _(i):
        @pl.when(i >= own)
        def _():
            wait_like(xbuf.at[0], rx.at[i - own])
        up_sample(0, i)

        @pl.when(lax.rem(i, 2) == 1)
        def _():
            tick(t0 + 2 + i // 2)
    arrived(k_u, k_d)

    @each(own)
    def _(i):
        wait_like(sbuf.at[0], sp.at[i])
        part_sample(0, i, trans_part)
        wait_like(xbuf.at[0], sx.at[i])

    @each(own)
    def _(i):
        resid_sample(0, 1, i, trans_part)
        ada_sample(1, 0, i)

        @pl.when(i < TAIL_TICKS - 4)
        def _():
            tick(t0 + 4 + i)
    wait_like(bqbuf.at[pl.ds(0, nx - 1)], r_bq)

    k_q, k_o, k_u, k_d = (need(g.lr + v, 0) for v in (g.o0, g.u0, g.d0, g.lr))
    first_k = need(g.lr, 0)

    def shard_of(q):
        return lax.rem(x + jnp.where(q == 0, 0, jnp.where(q == 1, nx - 1, q - 1)), nx)

    def rows_from(s):
        return lambda off, n: flat(s, 1, off, n)

    def q_bias1(s):
        return bqbuf[s].T[:lw, 1:2]

    def half_layer(hf, carry):
        def once(body):
            pl.when(hf == 0)(body)

        project(slot_a, xbuf[hf], rows_from(x), q_bias1(x))
        wait_like(xbuf.at[own + hf], rx.at[hf])

        def shard(q, inner):
            s = shard_of(q)
            after = shard_of(jnp.minimum(q + 1, nx - 1))
            bias_prep(rows_from(s))
            pair(slot_a, obuf.at[hf * nx + s], slot_b, xbuf[own + hf], rows_from(s), q_bias1(s))

            @pl.when(hf == 0)
            def _():
                tick(t1 + q)

                @pl.when(q == nx - 2)
                def _():
                    arrived(first_k, k_q)
            pair(slot_b, obuf.at[(own + hf) * nx + s], slot_a, xbuf[hf], rows_from(after), q_bias1(after))
            return inner
        lax.fori_loop(0, nx, shard, 0)
        once(lambda: arrived(k_q, k_o))
        pl.when(hf > 0)(lambda: out_relay(0))
        wait_like(sbuf.at[hf], sp.at[hf])
        part_sample(1, hf, attn_part)
        wait_like(xbuf.at[hf], sx.at[hf])
        resid_sample(1, 0, hf, attn_part)
        ada_sample(1, 1, hf)
        once(lambda: arrived(k_o, k_u))
        up_sample(1, hf)
        pl.when(hf > 0)(lambda: out_relay(1))
        wait_like(xbuf.at[own + hf], rx.at[hf])
        up_sample(1, own + hf)
        once(lambda: arrived(k_u, k_d))
        wait_like(sbuf.at[hf], sp.at[hf])
        part_sample(1, hf, trans_part)
        resid_sample(1, 1, hf, trans_part)
        out_first(hf)
        return carry

    lax.fori_loop(0, own, half_layer, 0)
    for i in range(own):
        wait_like(xbuf.at[i], sx.at[i])
        wait_like(sbuf.at[i], sp.at[i])
    for p in range(npc, own * npc):
        out_relay(p)
    for p in range(own * npc):
        oawait(2, o_d.at[p])
        opush(orow(tpo, p), dev_c, o_p2.at[p])
    for p in range(own * npc):
        oawait(2, o_p0.at[p])
        oawait(4, o_p1.at[p])
        oawait(2, o_p2.at[p])
    wait_like(out.at[pl.ds(0, 7 * own)], osend)
    wait_like(buf.at[pl.ds(0, 3)], send)
    wait_like(bqbuf.at[pl.ds(0, nx - 1)], s_bq)


def finish(src, dst, sem):
    cp = pltpu.make_async_copy(src, dst, sem)
    cp.start()
    cp.wait()


def solution(mesh):
    def body(token_act, token_cond, pair_bias, token_mask, ada_scale, ada_w, ada_bias, zero_w, zero_b, w_qkvg, b_q, w_o, w_up, w_down):
        g = Geometry(mesh, token_act.shape, token_cond.shape, pair_bias.shape, w_qkvg.shape, w_up.shape)
        L, D, C, T, own, nx = g.layers, g.width, g.cond_dim, g.tokens, g.own, g.nx
        ada = ada_w.transpose(0, 1, 3, 2, 4).reshape(2 * L, 2, C, D)
        zero = zero_w.transpose(0, 2, 1, 3).reshape(2 * L, C, D)
        vm = pl.BlockSpec(memory_space=pltpu.VMEM)
        hbm = pl.BlockSpec(memory_space=pl.ANY)
        dma = pltpu.SemaphoreType.DMA
        npc = own * (T // OUT_ROWS)
        K = g.chunks
        steps = nx * own
        gathered = pl.pallas_call(
            functools.partial(kernel, g),
            out_shape=pltpu.VMEM(token_act.shape, BF16),
            in_specs=[hbm, hbm, hbm, vm, vm, hbm, vm, hbm, vm, hbm, vm, hbm, hbm, hbm],
            out_specs=vm,
            scratch_shapes=[
                pltpu.VMEM((nx, g.rows, LANES), BF16),
                pltpu.VMEM((g.o0, LANES), BF16),
                pltpu.VMEM((2 * own, T, D), BF16),
                pltpu.VMEM((own, T, D), BF16),
                pltpu.VMEM((own, T, D), BF16),
                pltpu.VMEM((own, T, D), BF16),
                pltpu.VMEM((2 * own * nx + CORES * (steps - own), g.lw, T), BF16),
                pltpu.VMEM((2 * own, T, nx * g.hu), BF16),
                pltpu.VMEM((2 * own, T, C), BF16),
                pltpu.VMEM((own, T, C), BF16),
                pltpu.VMEM((own, T, C), F32),
                pltpu.VMEM((2 * L, 2, C, D), BF16),
                pltpu.VMEM((2 * L, C, D), BF16),
                pltpu.VMEM((nx, 8, LANES), F32),
                pltpu.VMEM((T, LANES), F32),
                pltpu.VMEM((g.heads, T, T), F32),
                pltpu.VMEM((g.lw, T), BF16),
                pltpu.VMEM((T, g.lw), BF16),
                pltpu.VMEM((g.lw, T), BF16),
                pltpu.VMEM((g.lw, T), F32),
                pltpu.VMEM((g.lw, T), BF16),
                pltpu.VMEM((T, g.lw), BF16),
                pltpu.VMEM((g.lw, T), BF16),
                pltpu.VMEM((g.lw, T), F32),
                dma((3,)), dma((3,)), dma, dma((4 * L,)), dma((2, 2 * own)), dma,
                dma((K,)), dma((K,)), dma((K,)), dma((K,)),
                dma, dma, dma, dma((steps,)), dma, dma, dma((CORES * own,)),
                dma((own,)), dma((own,)), dma((own,)), dma((own,)),
                dma, dma((npc,)), dma((npc,)), dma((npc,)), dma((npc,)), dma((npc,)),
            ],
            compiler_params=pltpu.CompilerParams(collective_id=0, has_side_effects=True, vmem_limit_bytes=207 << 18),
            name='blocks',
        )(token_act, token_cond, pair_bias, token_mask.reshape(1, T), ada_scale, ada, ada_bias, zero, zero_b, w_qkvg.transpose(0, 2, 3, 1), b_q, w_o, w_up.transpose(0, 2, 3, 1), w_down)
        gathered = pltpu.with_memory_space_constraint(gathered, pltpu.VMEM)
        return pl.pallas_call(
            finish,
            out_shape=jax.ShapeDtypeStruct(token_act.shape, BF16),
            in_specs=[vm],
            out_specs=pl.BlockSpec(memory_space=pltpu.HBM),
            scratch_shapes=[dma],
            compiler_params=pltpu.CompilerParams(vmem_limit_bytes=1 << 20),
            name='finish',
        )(gathered)

    everywhere = P()
    in_specs = (P('dp', None, None), P('dp', None, None), P(None, 'tp', None, None), P(None), everywhere, everywhere, everywhere, everywhere, everywhere, P(None, None, None, 'tp'), P(None, 'tp'), P(None, 'tp', None), P(None, None, None, 'tp'), P(None, 'tp', None))
    return jax.shard_map(body, mesh=mesh, in_specs=in_specs, out_specs=P('dp', None, None), check_vma=False)
```

```python
import functools
import math
import jax
import jax.numpy as jnp
from jax import lax
from jax.experimental import pallas as pl
from jax.experimental.pallas import tpu as pltpu
from jax.sharding import PartitionSpec as P

LN_EPS = 1e-5
LOG2E = 1.4426950408889634
MESH = pl.DeviceIdType.MESH
BF16 = jnp.bfloat16
F32 = jnp.float32
LANES = 128
CH = 1216
LA = 4
TAIL_TICKS = 6
HELD = 0
EARLY_LAG = 4
LAGS = (0, 2, 5)
RB = 512
OUT_ROWS = 256
CORES = 2
RING = 2


def dot_nt(lhs, rhs):
    return lax.dot_general(lhs, rhs, (((1,), (1,)), ((), ())), preferred_element_type=F32)


def dot_nn(lhs, rhs):
    return lax.dot_general(lhs, rhs, (((1,), (0,)), ((), ())), preferred_element_type=F32)


def normed(values_in):
    row_mean = jnp.mean(values_in, axis=-1, keepdims=True)
    centered = values_in - row_mean
    variance = jnp.mean(centered * centered, axis=-1, keepdims=True)
    return centered * lax.rsqrt(variance + LN_EPS)


class Geometry:
    def __init__(self, mesh, act, cond, bias, w_qkvg, w_up):
        self.nx = mesh.shape['tp'] // CORES
        self.y_stride = len({d.coords[2] for d in mesh.devices.flat})
        self.samples, self.tokens, self.width = act
        self.cond_dim = cond[-1]
        self.layers, self.heads = bias[0], bias[1]
        self.lw = w_qkvg[-1]
        self.hd = self.lw // self.heads
        self.hu = w_up[-1]
        self.own = self.samples // mesh.shape['tp']
        self.ncol = self.width // LANES
        self.tcol = self.tokens // LANES
        self.q0 = 0
        self.b0 = self.q0 + self.ncol * 4 * self.lw
        self.o0 = self.b0 + self.heads * self.tcol * self.tokens
        self.u0 = self.o0 + self.ncol * self.lw
        self.d0 = self.u0 + self.ncol * 2 * self.hu
        self.lr = self.d0 + self.ncol * self.hu
        self.flat_rows = self.layers * self.lr - self.o0
        self.chunks = -(-self.flat_rows // CH)
        self.rows = self.chunks * CH
        assert self.lw == 96 and self.hu == 192 and self.heads == 2 and self.nx == 4 and self.layers == 2 and self.own == 2


def kernel(g, act_in, cond_in, bias_in, mask_in, ascale_in, ada_in, abias_in, zero_in, zbias_in, wq_in, bq_in, wo_in, up_in, down_in,
           out, buf, qb0, xbuf, abuf, pbuf, sbuf, obuf, hbuf, cring, cbuf, lnbuf, adabuf, zerobuf, bqbuf, mcol, bmbuf, qa, ka, va, ga, qb, kb, vb, gb,
           s_loc, s_act, s_bias, s_ada, s_in, send, ra, rb, rc, rd, s_bq, r_bq, sx0, rx0, s_o, r_o, r_rel, sx, rx, sp, rp, osend, o_p0, o_a, o_p1, o_d, o_p2):
    nx, own, T, D = g.nx, g.own, g.tokens, g.width
    lw, hu, hd = g.lw, g.hu, g.hd
    half = hu - LANES
    tp = lax.axis_index('tp')
    dp = lax.axis_index('dp')
    x = tp // CORES
    c = lax.rem(tp, CORES)
    xp = lax.rem(x + 1, nx)
    xm = lax.rem(x + nx - 1, nx)
    xo = lax.rem(x + 2, nx)
    dev_p, dev_m, dev_o = ({'tp': v * CORES + c} for v in (xp, xm, xo))
    dev_c = {'tp': x * CORES + 1 - c}
    pz = lax.rem(dp, 2)
    py = lax.rem(dp // g.y_stride, 2)
    dev_z = {'dp': dp + 1 - 2 * pz}
    dev_y = {'dp': dp + g.y_stride * (1 - 2 * py)}
    mine = tp * own

    def remote(src, dst, s_sem, r_sem, dev):
        return pltpu.make_async_remote_copy(src, dst, s_sem, r_sem, device_id=dev, device_id_type=MESH)

    def wait_like(ref, sem):
        pltpu.make_async_copy(ref, ref, sem).wait()

    barrier = pltpu.get_barrier_semaphore()
    devs = (dev_p, dev_m, dev_o, dev_c, dev_z, dev_y)
    for d in devs:
        pl.semaphore_signal(barrier, inc=1, device_id=d, device_id_type=MESH)

    steps = nx * own

    def chip_of(n):
        near = jnp.where(lax.rem(n, 2) == 0, 1, nx - 1)
        return lax.rem(x + jnp.where(n < own, 2, jnp.where(n < 3 * own, near, 0)), nx)

    def pair_of(n):
        return jnp.where((n < own) | (n >= 3 * own), lax.rem(n, own), (n - own) // 2)

    def sample_of(n, core):
        return chip_of(n) * (CORES * own) + pair_of(n) * CORES + core

    def load_sample(n):
        slot = lax.rem(n, RING)
        pltpu.make_async_copy(act_in.at[sample_of(n, c)], hbuf.at[slot], s_in.at[0, slot]).start()
        pltpu.make_async_copy(cond_in.at[sample_of(n, c)], cring.at[slot], s_in.at[1, slot]).start()

    load_sample(0)
    ada_cps = [pltpu.make_async_copy(ada_in.at[v], adabuf.at[v], s_ada.at[v]) for v in range(2 * g.layers)]
    zero_cps = [pltpu.make_async_copy(zero_in.at[v], zerobuf.at[v], s_ada.at[2 * g.layers + v]) for v in range(2 * g.layers)]
    ada_cps[0].start()

    u_parts = ((0, 0, LANES, 0), (0, LANES, half, LANES), (1, LANES, half, LANES + half), (1, 0, LANES, 2 * LANES))

    def load_attn(l, place, sem):
        for j in range(g.ncol):
            for f in range(4):
                pltpu.make_async_copy(wq_in.at[l, f, :, pl.ds(j * LANES, LANES)], place(g.q0 + (j * 4 + f) * lw, lw), sem).start()

    def load_bias(l):
        for h in range(g.heads):
            pltpu.make_async_copy(bias_in.at[l, h], abuf.at[h, :, pl.ds(0, T)], s_bias).start()

    def turn_bias(l, put):
        for h in range(g.heads):
            wait_like(abuf.at[h, :, pl.ds(0, T)], s_bias)
        for h in range(g.heads):
            for j in range(g.tcol):
                put(g.b0 + (h * g.tcol + j) * T, abuf[h, pl.ds(j * LANES, LANES), pl.ds(0, T)].T)

    def load_rest(l, place, sem):
        for j in range(g.ncol):
            col = pl.ds(j * LANES, LANES)
            pltpu.make_async_copy(wo_in.at[l, :, col], place(g.o0 + j * lw, lw), sem).start()
            for f, r0, n, off in u_parts:
                pltpu.make_async_copy(up_in.at[l, f, pl.ds(r0, n), col], place(g.u0 + j * 2 * hu + off, n), sem).start()
            pltpu.make_async_copy(down_in.at[l, :, col], place(g.d0 + j * hu, hu), sem).start()

    def own_rows(l):
        return lambda off, n: buf.at[x, pl.ds(l * g.lr - g.o0 + off, n)]

    load_bias(0)
    load_rest(0, own_rows(0), s_loc.at[1])
    act_cp = pltpu.make_async_copy(act_in.at[pl.ds(mine, own)], abuf, s_act.at[0])
    cond_cp = pltpu.make_async_copy(cond_in.at[pl.ds(mine, own)], cbuf, s_act.at[1])
    bqbuf[x] = jnp.zeros((8, LANES), F32)
    bqbuf[x, pl.ds(0, g.layers), pl.ds(0, lw)] = bq_in[...]

    pad = g.rows - g.flat_rows
    if pad:
        buf[x, pl.ds(g.flat_rows, pad), :] = jnp.zeros((pad, LANES), BF16)

    Q = CH // 4
    g0 = 2 * py + pz
    gy = 2 * (1 - py) + pz
    gz = 2 * py + 1 - pz
    gd = 2 * (1 - py) + 1 - pz

    def push(blk, k, part, dev, r_sem):
        r = buf.at[blk, pl.ds(pl.multiple_of(k * CH + part * Q, 8), Q)]
        remote(r, r, send, r_sem, dev).start()

    def await_quarters(n, sem):
        wait_like(buf.at[0, pl.ds(0, n * Q)], sem)

    def first(k):
        push(x, k, g0, dev_p, ra.at[k])
        push(x, k, g0, dev_m, ra.at[k])

    def stage1(k):
        await_quarters(2, ra.at[k])
        for blk in (xm, xp):
            push(blk, k, g0, dev_y, rb.at[k])
            push(blk, k, g0, dev_z, rb.at[k])

    def stage2(k):
        await_quarters(4, rb.at[k])
        push(xm, k, gz, dev_y, rc.at[k])
        push(xp, k, gy, dev_z, rc.at[k])

    def stage3(k):
        await_quarters(2, rc.at[k])
        for part in (g0, gy):
            push(xm, k, part, dev_p, rd.at[k])
        for part in (gz, gd):
            push(xp, k, part, dev_m, rd.at[k])

    def stage4(k):
        await_quarters(4, rd.at[k])

    K = g.chunks

    def tick(t):
        @pl.when(t + LA < K)
        def _():
            first(t + LA)
        split = need(g.lr, 0)
        for lag, stage, lo, hi in ((LAGS[0], stage1, 0, K), (LAGS[1], stage2, 0, K), (EARLY_LAG, stage3, 0, split), (LAGS[2], stage3, split, K)):
            @pl.when((t - lag >= lo) & (t - lag < hi))
            def _(lag=lag, stage=stage):
                stage(t - lag)

    def need(rows_end, lag):
        return -(-(rows_end - g.o0) // CH) + lag

    lane = lax.broadcasted_iota(jnp.int32, (1, LANES), 1)
    scale2 = LOG2E / math.sqrt(hd)

    def modulated(l, j, cond_ln, act_of):
        c_in = (cond_ln * ascale_in[l, pl.ds(j, 1), :]).astype(BF16)
        gain = jax.nn.sigmoid(dot_nn(c_in, adabuf[l * 2 + j, 0]) + abias_in[l, pl.ds(j, 1), :])
        shift = dot_nn(c_in, adabuf[l * 2 + j, 1])
        return (gain * normed(act_of().astype(F32)) + shift).astype(BF16)

    def row_blocks(body):
        for r in range(T // RB):
            body(pl.ds(r * RB, RB))

    full = pl.ds(0, T)

    def ada_rows(l, j, i, rows, n=0):
        xbuf[i, rows, :] = modulated(l, j, lnbuf[i, rows, :], lambda: abuf[i, rows, :])
        remote(xbuf.at[i, rows], xbuf.at[own + i, rows], sx.at[i, n], rx.at[i, n], dev_c).start()

    def resid_rows(l, j, i, part_of, rows, n=0):
        ours = part_of(l, i, rows)
        gate = jax.nn.sigmoid(dot_nn(cbuf[i, rows, :], zerobuf[l * 2 + j]) + zbias_in[l, pl.ds(j, 1), :])
        wait_like(pbuf.at[i, rows], rp.at[i, n])
        act = (abuf[i, rows, :].astype(F32) + gate * (ours + pbuf[i, rows, :].astype(F32)).astype(BF16).astype(F32)).astype(BF16)
        abuf[i, rows, :] = act
        if j == 1:
            out[mine + i, rows, :] = act

    def part_rows(l, i, part_of, rows, n=0):
        sbuf[i, rows, :] = part_of(l, own + i, rows).astype(BF16)
        remote(sbuf.at[i, rows], pbuf.at[i, rows], sp.at[i, n], rp.at[i, n], dev_c).start()

    stage0 = 2 * own * nx

    def relay_box(v):
        return xbuf.at[v, pl.ds(0, lw), pl.ds(0, T)]

    def flat(s, l, off, n):
        return buf[s, pl.ds(pl.multiple_of(l * g.lr - g.o0 + off, 8), n), :]

    def bias_prep(rows_of):
        for h in range(g.heads):
            for j in range(g.tcol):
                col = pl.ds(j * LANES, LANES)
                bmbuf[h, :, col] = rows_of(g.b0 + (h * g.tcol + j) * T, T).astype(F32) * LOG2E + mcol[...]

    def project_dot(x_rows, rows_of):
        w = jnp.concatenate([rows_of(g.q0 + j * 4 * lw, 4 * lw) for j in range(g.ncol)], axis=1)
        return dot_nt(w, x_rows)

    def project_end(slot, proj, q_bias):
        qs, ks, vs, gs = slot
        qs[...] = (proj[:lw] + q_bias).astype(BF16)
        ks[...] = proj[lw:2 * lw].astype(BF16).T
        vs[...] = proj[2 * lw:3 * lw].astype(BF16)
        gs[...] = jax.nn.sigmoid(proj[3 * lw:])

    def scores(slot, h):
        qs, ks, _, _ = slot
        none = jnp.zeros((hd, T), BF16)
        q = jnp.concatenate([qs[pl.ds(h * hd, hd), :] if v == h else none for v in range(g.heads)], axis=0)
        return dot_nn(ks[...], q)

    def weights(h, s):
        z = s * scale2 + bmbuf[h]
        return jnp.exp2(z - jnp.max(z, axis=0, keepdims=True)).astype(BF16)

    def mix(slot, h, e, o_ref):
        _, _, vs, gs = slot
        mine_h = pl.ds(h * hd, hd)
        o = dot_nn(jnp.concatenate([vs[mine_h, :], jnp.ones((16, T), BF16)], axis=0), e)
        o_ref[mine_h, :] = (o[:hd] * (1.0 / o[hd:hd + 1]) * gs[mine_h, :]).astype(BF16)

    def project(slot, x_rows, rows_of, q_bias):
        project_end(slot, project_dot(x_rows, rows_of), q_bias)

    def pair(slot, o_ref, after, x_rows, rows_of, q_bias):
        s0 = scores(slot, 0)
        s1 = scores(slot, 1)
        proj = project_dot(x_rows, rows_of)
        e0 = weights(0, s0)
        mix(slot, 0, e0, o_ref)
        e1 = weights(1, s1)
        mix(slot, 1, e1, o_ref)
        project_end(after, proj, q_bias)
    slot_a = (qa, ka, va, ga)
    slot_b = (qb, kb, vb, gb)

    def ada_first(n):
        slot = lax.rem(n, RING)
        s = sample_of(n, c)
        wait_like(hbuf.at[slot], s_in.at[0, slot])
        wait_like(cring.at[slot], s_in.at[1, slot])
        def rows_body(rows):
            out[s, rows, :] = modulated(0, 0, normed(cring[slot, rows, :].astype(F32)), lambda: hbuf[slot, rows, :])
        row_blocks(rows_body)
        remote(out.at[s], out.at[s], sx0, rx0.at[n], dev_c).start()
        @pl.when(n + RING < steps)
        def _():
            load_sample(n + RING)

    def qb_rows(off, n):
        return qb0[pl.ds(off, n), :]

    ada_cps[0].wait()
    load_attn(0, lambda off, n: qb0.at[pl.ds(off, n)], s_loc.at[0])
    for n in range(1, RING):
        load_sample(n)
    load_attn(1, own_rows(1), s_loc.at[2])
    load_rest(1, own_rows(1), s_loc.at[2])
    for cp in (cond_cp, zero_cps[0], *ada_cps[1:], *zero_cps[1:]):
        cp.start()
    pl.semaphore_wait(barrier, len(devs))
    wait_like(buf.at[x, pl.ds(0, g.lr - g.o0)], s_loc.at[1])
    early = (g.lr - g.o0) // CH
    for k in range(min(LA, early)):
        first(k)
    ada_first(0)
    mask_col = jnp.broadcast_to((mask_in[...].astype(F32) - 1.0) * (1e9 * LOG2E), (8, T)).T
    mcol[...] = jnp.broadcast_to(mask_col[:, 0:1], (T, LANES))

    def put_first(off, v):
        qb0[pl.ds(off, T), :] = v
    turn_bias(0, put_first)
    load_bias(1)
    wait_like(qb0.at[pl.ds(0, g.b0)], s_loc.at[0])
    bias_prep(qb_rows)
    for d in (dev_p, dev_m, dev_o):
        remote(bqbuf.at[x], bqbuf.at[x], s_bq, r_bq, d).start()
    q_bias0 = bqbuf[x].T[:lw, 0:1]
    project(slot_a, out[sample_of(0, c)], qb_rows, q_bias0)
    wait_like(buf.at[x, pl.ds(0, g.lr - g.o0 + g.b0)], s_loc.at[2])
    for k in range(min(LA, early), LA):
        first(k)

    def put_second(off, v):
        buf[x, pl.ds(g.lr - g.o0 + off, T), :] = v

    def first_steps(m, carry):
        @pl.when(m == 1)
        def _():
            turn_bias(1, put_second)
            act_cp.start()

        @pl.when(m + 1 < steps)
        def _():
            ada_first(m + 1)

        def slot_of(pair, core):
            return jnp.where(pair == c, 0, own) + core

        def place_of(u, core):
            slot = slot_of(pair_of(m), core) * nx + x
            return slot, jnp.where(m < steps - own, stage0 + CORES * m + u, slot)

        def send(u, slot, place):
            @pl.when(m == 0)
            def _():
                remote(obuf.at[place], relay_box(u), s_o, r_rel.at[u], dev_p).start()

            @pl.when(m == 1)
            def _():
                remote(obuf.at[place], relay_box(CORES + u), s_o, r_rel.at[CORES + u], dev_m).start()

            @pl.when((m >= own) & (m < steps - own))
            def _():
                remote(obuf.at[place], obuf.at[slot], s_o, r_o, {'tp': chip_of(m) * CORES + c}).start()

        def forward(pair, dev, source):
            for u, core in enumerate((c, 1 - c)):
                r = relay_box(pair * CORES + u)
                wait_like(r, r_rel.at[pair * CORES + u])
                remote(r, obuf.at[slot_of(pair, core) * nx + source], s_o, r_o, dev).start()

        @pl.when(m == own + 1)
        def _():
            forward(0, dev_p, xm)

        @pl.when(m == own + 2)
        def _():
            forward(1, dev_m, xp)
        wait_like(out.at[0], rx0.at[m])
        slot, place = place_of(0, c)
        pair(slot_a, obuf.at[place], slot_b, out[sample_of(m, 1 - c)], qb_rows, q_bias0)
        send(0, slot, place)
        slot, place = place_of(1, 1 - c)
        pair(slot_b, obuf.at[place], slot_a, out[sample_of(jnp.minimum(m + 1, steps - 1), c)], qb_rows, q_bias0)
        send(1, slot, place)

        @pl.when(m >= HELD)
        def _():
            tick(m - HELD)
        return carry
    lax.fori_loop(0, steps, first_steps, 0)

    cond_cp.wait()
    act_cp.wait()
    for i in range(own):
        lnbuf[i] = normed(cbuf[i].astype(F32))
    for cp in (*ada_cps[1:], *zero_cps):
        cp.wait()
    remote_pieces = CORES * (steps - own)
    wait_like(obuf.at[pl.ds(stage0, remote_pieces)], r_o)
    wait_like(obuf.at[pl.ds(0, remote_pieces + CORES * own)], s_o)
    wait_like(out.at[pl.ds(0, steps)], sx0)

    def attn_part(l, i, rows):
        lhs = jnp.concatenate([obuf[i * nx + s, :, rows] for s in range(nx)], axis=0)
        rhs = jnp.concatenate([jnp.concatenate([flat(s, l, g.o0 + j * lw, lw) for s in range(nx)], axis=0) for j in range(g.ncol)], axis=1)
        return lax.dot_general(lhs, rhs, (((0,), (0,)), ((), ())), preferred_element_type=F32)

    def up_rows(l, i, rows=full):
        y = xbuf[i, rows, :]
        pre = []
        for p in range(nx // 2):
            w = jnp.concatenate([jnp.concatenate([flat(2 * p + e, l, g.u0 + j * 2 * hu, 2 * hu) for j in range(g.ncol)], axis=1) for e in range(2)], axis=0)
            pre.append(dot_nt(y, w))
        for p in range(nx // 2):
            mids = []
            for e in range(2):
                ua, ub, uc = (pre[p][:, (3 * e + v) * LANES:(3 * e + v + 1) * LANES] for v in range(3))
                side = (3 * p + 2 * e) * LANES
                hbuf[i, rows, side:side + LANES] = (jax.nn.silu(ua) * uc).astype(BF16)
                act = jax.nn.silu(ub)
                mids.append(act * pltpu.roll(ub, half, 1) if e == 0 else pltpu.roll(act, half, 1) * ub)
            mid = (3 * p + 1) * LANES
            hbuf[i, rows, mid:mid + LANES] = jnp.where(lane < half, mids[0], mids[1]).astype(BF16)

    def trans_part(l, i, rows):
        cols = []
        for j in range(g.ncol):
            v = []
            for p in range(nx // 2):
                v.append(flat(2 * p, l, g.d0 + j * hu, hu))
                v.append(flat(2 * p + 1, l, g.d0 + j * hu + LANES, half))
                v.append(flat(2 * p + 1, l, g.d0 + j * hu, LANES))
            cols.append(jnp.concatenate(v, axis=0))
        return dot_nn(hbuf[i, rows, :], jnp.concatenate(cols, axis=1))

    PR = OUT_ROWS
    npc = T // PR
    tpp, tpm, tpo = (v * CORES + c for v in (xp, xm, xo))

    def orow(blk, p, lo=0, n=PR):
        return out.at[blk * own + p // npc, pl.ds(pl.multiple_of(lax.rem(p, npc) * PR, PR) + lo, n)]

    def opush(r, dev, sem):
        remote(r, r, osend, sem, dev).start()

    def oawait(halves, sem):
        wait_like(out.at[0, pl.ds(0, halves * PR // 2)], sem)

    def out_first(p):
        opush(orow(tp, p), dev_p, o_a.at[p])
        opush(orow(tp, p), dev_m, o_a.at[p])
        opush(orow(tp, p), dev_c, o_p0.at[p])

    def out_relay(p):
        oawait(4, o_a.at[p])
        opush(orow(tpm, p, 0, PR // 2), dev_p, o_d.at[p])
        opush(orow(tpp, p, PR // 2, PR // 2), dev_m, o_d.at[p])
        opush(orow(tpm, p), dev_c, o_p1.at[p])
        opush(orow(tpp, p), dev_c, o_p1.at[p])

    t0 = steps - HELD
    t1 = t0 + TAIL_TICKS
    assert K + LAGS[-1] <= t1 + nx and need(g.d0, LAGS[-1]) <= t0 + 2 and need(g.lr, LAGS[-1]) <= t0 + 4
    assert need(g.lr + g.o0, LAGS[-1]) <= t1 + nx - 1 and need(g.lr + g.o0, LAGS[2]) <= t1

    def arrived(lo, hi):
        for k in range(lo, hi):
            stage4(k)

    k_o, k_u, k_d = (need(v, 0) for v in (g.u0, g.d0, g.lr))
    def each(count):
        def run(body):
            def step(i, carry):
                body(i)
                return carry
            lax.fori_loop(0, count, step, 0)
        return run

    arrived(0, k_o)

    @each(own)
    def _(i):
        part_rows(0, i, attn_part, full)

    @each(own)
    def _(i):
        resid_rows(0, 0, i, attn_part, full)
        ada_rows(0, 1, i, full)
        tick(t0 + i)
    arrived(k_o, k_u)

    @each(2 * own)
    def _(i):
        @pl.when(i >= own)
        def _():
            wait_like(xbuf.at[0], rx.at[i - own, 0])
        up_rows(0, i)

        @pl.when(lax.rem(i, 2) == 1)
        def _():
            tick(t0 + 2 + i // 2)
    arrived(k_u, k_d)

    @each(own)
    def _(i):
        wait_like(sbuf.at[0], sp.at[i, 0])
        part_rows(0, i, trans_part, full)
        wait_like(xbuf.at[0], sx.at[i, 0])

    @each(own)
    def _(i):
        resid_rows(0, 1, i, trans_part, full)
        ada_rows(1, 0, i, full)

        @pl.when(i < TAIL_TICKS - 4)
        def _():
            tick(t0 + 4 + i)
    wait_like(bqbuf.at[pl.ds(0, nx - 1)], r_bq)

    k_q, k_o, k_u, k_d = (need(g.lr + v, 0) for v in (g.o0, g.u0, g.d0, g.lr))
    first_k = need(g.lr, 0)

    def shard_of(q):
        return lax.rem(x + jnp.where(q == 0, 0, jnp.where(q == 1, nx - 1, q - 1)), nx)

    def rows_from(s):
        return lambda off, n: flat(s, 1, off, n)

    def q_bias1(s):
        return bqbuf[s].T[:lw, 1:2]

    def half_layer(hf, carry):
        def once(body):
            pl.when(hf == 0)(body)

        project(slot_a, xbuf[hf], rows_from(x), q_bias1(x))
        wait_like(xbuf.at[own + hf], rx.at[hf, 0])

        def shard(q, inner):
            s = shard_of(q)
            after = shard_of(jnp.minimum(q + 1, nx - 1))
            bias_prep(rows_from(s))
            pl.when((hf > 0) & (q == nx - 1))(lambda: out_relay(0))
            pair(slot_a, obuf.at[hf * nx + s], slot_b, xbuf[own + hf], rows_from(s), q_bias1(s))

            @pl.when(hf == 0)
            def _():
                tick(t1 + q)

                @pl.when(q == nx - 2)
                def _():
                    arrived(first_k, k_q)
            pair(slot_b, obuf.at[(own + hf) * nx + s], slot_a, xbuf[hf], rows_from(after), q_bias1(after))
            return inner
        lax.fori_loop(0, nx, shard, 0)
        once(lambda: arrived(k_q, k_o))
        ha, hb = (pl.ds(v * PR, PR) for v in range(2))
        wait_like(sbuf.at[hf], sp.at[hf, 0])
        wait_like(xbuf.at[hf], sx.at[hf, 0])
        part_rows(1, hf, attn_part, ha, 0)
        part_rows(1, hf, attn_part, hb, 1)
        resid_rows(1, 0, hf, attn_part, ha, 0)
        ada_rows(1, 1, hf, ha, 0)
        once(lambda: arrived(k_o, k_u))
        up_rows(1, hf, ha)
        resid_rows(1, 0, hf, attn_part, hb, 1)
        ada_rows(1, 1, hf, hb, 1)
        wait_like(xbuf.at[own + hf, ha], rx.at[hf, 0])
        up_rows(1, own + hf, ha)
        once(lambda: arrived(k_u, k_d))
        wait_like(sbuf.at[hf, ha], sp.at[hf, 0])
        part_rows(1, hf, trans_part, ha, 0)
        up_rows(1, hf, hb)
        pl.when(hf > 0)(lambda: out_relay(1))
        resid_rows(1, 1, hf, trans_part, ha, 0)
        out_first(hf * npc)
        wait_like(xbuf.at[own + hf, hb], rx.at[hf, 1])
        up_rows(1, own + hf, hb)
        wait_like(sbuf.at[hf, hb], sp.at[hf, 1])
        part_rows(1, hf, trans_part, hb, 1)
        resid_rows(1, 1, hf, trans_part, hb, 1)
        out_first(hf * npc + 1)
        for n, rows in enumerate((ha, hb)):
            wait_like(xbuf.at[hf, rows], sx.at[hf, n])
            wait_like(sbuf.at[hf, rows], sp.at[hf, n])
        return carry

    lax.fori_loop(0, own, half_layer, 0)
    for p in range(npc, own * npc):
        out_relay(p)
    for p in range(own * npc):
        oawait(2, o_d.at[p])
        opush(orow(tpo, p), dev_c, o_p2.at[p])
    for p in range(own * npc):
        oawait(2, o_p0.at[p])
        oawait(4, o_p1.at[p])
        oawait(2, o_p2.at[p])
    wait_like(out.at[pl.ds(0, 7 * own)], osend)
    wait_like(buf.at[pl.ds(0, 3)], send)
    wait_like(bqbuf.at[pl.ds(0, nx - 1)], s_bq)


def finish(src, dst, sem):
    cps = [pltpu.make_async_copy(src.at[v], dst.at[v], sem.at[v]) for v in range(src.shape[0])]
    for cp in cps:
        cp.start()
    for cp in cps:
        cp.wait()


def solution(mesh):
    def body(token_act, token_cond, pair_bias, token_mask, ada_scale, ada_w, ada_bias, zero_w, zero_b, w_qkvg, b_q, w_o, w_up, w_down):
        g = Geometry(mesh, token_act.shape, token_cond.shape, pair_bias.shape, w_qkvg.shape, w_up.shape)
        L, D, C, T, own, nx = g.layers, g.width, g.cond_dim, g.tokens, g.own, g.nx
        ada = ada_w.transpose(0, 1, 3, 2, 4).reshape(2 * L, 2, C, D)
        zero = zero_w.transpose(0, 2, 1, 3).reshape(2 * L, C, D)
        vm = pl.BlockSpec(memory_space=pltpu.VMEM)
        hbm = pl.BlockSpec(memory_space=pl.ANY)
        dma = pltpu.SemaphoreType.DMA
        npc = own * (T // OUT_ROWS)
        K = g.chunks
        steps = nx * own
        gathered = pl.pallas_call(
            functools.partial(kernel, g),
            out_shape=pltpu.VMEM(token_act.shape, BF16),
            in_specs=[hbm, hbm, hbm, vm, vm, hbm, vm, hbm, vm, hbm, vm, hbm, hbm, hbm],
            out_specs=vm,
            scratch_shapes=[
                pltpu.VMEM((nx, g.rows, LANES), BF16),
                pltpu.VMEM((g.o0, LANES), BF16),
                pltpu.VMEM((2 * own, T, D), BF16),
                pltpu.VMEM((own, T, D), BF16),
                pltpu.VMEM((own, T, D), BF16),
                pltpu.VMEM((own, T, D), BF16),
                pltpu.VMEM((2 * own * nx + CORES * (steps - own), g.lw, T), BF16),
                pltpu.VMEM((2 * own, T, nx * g.hu), BF16),
                pltpu.VMEM((RING, T, C), BF16),
                pltpu.VMEM((own, T, C), BF16),
                pltpu.VMEM((own, T, C), F32),
                pltpu.VMEM((2 * L, 2, C, D), BF16),
                pltpu.VMEM((2 * L, C, D), BF16),
                pltpu.VMEM((nx, 8, LANES), F32),
                pltpu.VMEM((T, LANES), F32),
                pltpu.VMEM((g.heads, T, T), F32),
                pltpu.VMEM((g.lw, T), BF16),
                pltpu.VMEM((T, g.lw), BF16),
                pltpu.VMEM((g.lw, T), BF16),
                pltpu.VMEM((g.lw, T), F32),
                pltpu.VMEM((g.lw, T), BF16),
                pltpu.VMEM((T, g.lw), BF16),
                pltpu.VMEM((g.lw, T), BF16),
                pltpu.VMEM((g.lw, T), F32),
                dma((3,)), dma((3,)), dma, dma((4 * L,)), dma((2, RING)), dma,
                dma((K,)), dma((K,)), dma((K,)), dma((K,)),
                dma, dma, dma, dma((steps,)), dma, dma, dma((CORES * own,)),
                dma((own, 2)), dma((own, 2)), dma((own, 2)), dma((own, 2)),
                dma, dma((npc,)), dma((npc,)), dma((npc,)), dma((npc,)), dma((npc,)),
            ],
            compiler_params=pltpu.CompilerParams(collective_id=0, has_side_effects=True, vmem_limit_bytes=207 << 18),
            name='blocks',
        )(token_act, token_cond, pair_bias, token_mask.reshape(1, T), ada_scale, ada, ada_bias, zero, zero_b, w_qkvg.transpose(0, 2, 3, 1), b_q, w_o, w_up.transpose(0, 2, 3, 1), w_down)
        gathered = pltpu.with_memory_space_constraint(gathered, pltpu.VMEM)
        return pl.pallas_call(
            finish,
            out_shape=jax.ShapeDtypeStruct(token_act.shape, BF16),
            in_specs=[vm],
            out_specs=pl.BlockSpec(memory_space=pltpu.HBM),
            scratch_shapes=[dma((token_act.shape[0],))],
            compiler_params=pltpu.CompilerParams(vmem_limit_bytes=1 << 20),
            name='finish',
        )(gathered)

    everywhere = P()
    in_specs = (P('dp', None, None), P('dp', None, None), P(None, 'tp', None, None), P(None), everywhere, everywhere, everywhere, everywhere, everywhere, P(None, None, None, 'tp'), P(None, 'tp'), P(None, 'tp', None), P(None, None, None, 'tp'), P(None, 'tp', None))
    return jax.shard_map(body, mesh=mesh, in_specs=in_specs, out_specs=P('dp', None, None), check_vma=False)
```

```python
import functools
import math
import jax
import jax.numpy as jnp
from jax import lax
from jax.experimental import pallas as pl
from jax.experimental.pallas import tpu as pltpu
from jax.sharding import PartitionSpec as P

LN_EPS = 1e-5
LOG2E = 1.4426950408889634
MESH = pl.DeviceIdType.MESH
BF16 = jnp.bfloat16
F32 = jnp.float32
LANES = 128
CH = 1216
LA = 4
TAIL_TICKS = 6
HELD = 0
EARLY_LAG = 4
LAGS = (0, 2, 5)
RB = 512
OUT_ROWS = 256
CORES = 2
RING = 2


def dot_nt(lhs, rhs):
    return lax.dot_general(lhs, rhs, (((1,), (1,)), ((), ())), preferred_element_type=F32)


def dot_nn(lhs, rhs):
    return lax.dot_general(lhs, rhs, (((1,), (0,)), ((), ())), preferred_element_type=F32)


def normed(values_in):
    row_mean = jnp.mean(values_in, axis=-1, keepdims=True)
    centered = values_in - row_mean
    variance = jnp.mean(centered * centered, axis=-1, keepdims=True)
    return centered * lax.rsqrt(variance + LN_EPS)


class Geometry:
    def __init__(self, mesh, act, cond, bias, w_qkvg, w_up):
        self.nx = mesh.shape['tp'] // CORES
        self.y_stride = len({d.coords[2] for d in mesh.devices.flat})
        self.samples, self.tokens, self.width = act
        self.cond_dim = cond[-1]
        self.layers, self.heads = bias[0], bias[1]
        self.lw = w_qkvg[-1]
        self.hd = self.lw // self.heads
        self.hu = w_up[-1]
        self.own = self.samples // mesh.shape['tp']
        self.ncol = self.width // LANES
        self.tcol = self.tokens // LANES
        self.q0 = 0
        self.b0 = self.q0 + self.ncol * 4 * self.lw
        self.o0 = self.b0 + self.heads * self.tcol * self.tokens
        self.u0 = self.o0 + self.ncol * self.lw
        self.d0 = self.u0 + self.ncol * 2 * self.hu
        self.lr = self.d0 + self.ncol * self.hu
        self.flat_rows = self.layers * self.lr - self.o0
        self.chunks = -(-self.flat_rows // CH)
        self.rows = self.chunks * CH
        assert self.lw == 96 and self.hu == 192 and self.heads == 2 and self.nx == 4 and self.layers == 2 and self.own == 2


def kernel(g, act_in, cond_in, bias_in, mask_in, ascale_in, ada_in, abias_in, zero_in, zbias_in, wq_in, bq_in, wo_in, up_in, down_in,
           out, buf, qb0, xbuf, abuf, pbuf, sbuf, obuf, hbuf, cring, cbuf, lnbuf, adabuf, zerobuf, bqbuf, mcol, bmbuf, qa, ka, va, ga, qb, kb, vb, gb,
           s_loc, s_act, s_bias, s_ada, s_in, send, ra, rb, rc, rd, s_bq, r_bq, sx0, rx0, s_o, r_o, r_rel, sx, rx, sp, rp, osend, o_p0, o_a, o_p1, o_d, o_p2):
    nx, own, T, D = g.nx, g.own, g.tokens, g.width
    lw, hu, hd = g.lw, g.hu, g.hd
    half = hu - LANES
    tp = lax.axis_index('tp')
    dp = lax.axis_index('dp')
    x = tp // CORES
    c = lax.rem(tp, CORES)
    xp = lax.rem(x + 1, nx)
    xm = lax.rem(x + nx - 1, nx)
    xo = lax.rem(x + 2, nx)
    dev_p, dev_m, dev_o = ({'tp': v * CORES + c} for v in (xp, xm, xo))
    dev_c = {'tp': x * CORES + 1 - c}
    pz = lax.rem(dp, 2)
    py = lax.rem(dp // g.y_stride, 2)
    dev_z = {'dp': dp + 1 - 2 * pz}
    dev_y = {'dp': dp + g.y_stride * (1 - 2 * py)}
    mine = tp * own

    def remote(src, dst, s_sem, r_sem, dev):
        return pltpu.make_async_remote_copy(src, dst, s_sem, r_sem, device_id=dev, device_id_type=MESH)

    def wait_like(ref, sem):
        pltpu.make_async_copy(ref, ref, sem).wait()

    barrier = pltpu.get_barrier_semaphore()
    devs = (dev_p, dev_m, dev_o, dev_c, dev_z, dev_y)
    for d in devs:
        pl.semaphore_signal(barrier, inc=1, device_id=d, device_id_type=MESH)

    steps = nx * own

    def chip_of(n):
        near = jnp.where(lax.rem(n, 2) == 0, 1, nx - 1)
        return lax.rem(x + jnp.where(n < own, 2, jnp.where(n < 3 * own, near, 0)), nx)

    def pair_of(n):
        return jnp.where((n < own) | (n >= 3 * own), lax.rem(n, own), (n - own) // 2)

    def sample_of(n, core):
        return chip_of(n) * (CORES * own) + pair_of(n) * CORES + core

    def load_sample(n):
        slot = lax.rem(n, RING)
        pltpu.make_async_copy(act_in.at[sample_of(n, c)], hbuf.at[slot], s_in.at[0, slot]).start()
        pltpu.make_async_copy(cond_in.at[sample_of(n, c)], cring.at[slot], s_in.at[1, slot]).start()

    load_sample(0)
    ada_cps = [pltpu.make_async_copy(ada_in.at[v], adabuf.at[v], s_ada.at[v]) for v in range(2 * g.layers)]
    zero_cps = [pltpu.make_async_copy(zero_in.at[v], zerobuf.at[v], s_ada.at[2 * g.layers + v]) for v in range(2 * g.layers)]
    ada_cps[0].start()

    u_parts = ((0, 0, LANES, 0), (0, LANES, half, LANES), (1, LANES, half, LANES + half), (1, 0, LANES, 2 * LANES))

    def load_attn(l, place, sem):
        for j in range(g.ncol):
            for f in range(4):
                pltpu.make_async_copy(wq_in.at[l, f, :, pl.ds(j * LANES, LANES)], place(g.q0 + (j * 4 + f) * lw, lw), sem).start()

    def load_bias(l):
        for h in range(g.heads):
            pltpu.make_async_copy(bias_in.at[l, h], abuf.at[h, :, pl.ds(0, T)], s_bias).start()

    def turn_bias(l, put):
        for h in range(g.heads):
            wait_like(abuf.at[h, :, pl.ds(0, T)], s_bias)
        for h in range(g.heads):
            for j in range(g.tcol):
                put(g.b0 + (h * g.tcol + j) * T, abuf[h, pl.ds(j * LANES, LANES), pl.ds(0, T)].T)

    def load_rest(l, place, sem):
        for j in range(g.ncol):
            col = pl.ds(j * LANES, LANES)
            pltpu.make_async_copy(wo_in.at[l, :, col], place(g.o0 + j * lw, lw), sem).start()
            for f, r0, n, off in u_parts:
                pltpu.make_async_copy(up_in.at[l, f, pl.ds(r0, n), col], place(g.u0 + j * 2 * hu + off, n), sem).start()
            pltpu.make_async_copy(down_in.at[l, :, col], place(g.d0 + j * hu, hu), sem).start()

    def own_rows(l):
        return lambda off, n: buf.at[x, pl.ds(l * g.lr - g.o0 + off, n)]

    load_bias(0)
    load_rest(0, own_rows(0), s_loc.at[1])
    act_cp = pltpu.make_async_copy(act_in.at[pl.ds(mine, own)], abuf, s_act.at[0])
    cond_cp = pltpu.make_async_copy(cond_in.at[pl.ds(mine, own)], cbuf, s_act.at[1])
    bqbuf[x] = jnp.zeros((8, LANES), F32)
    bqbuf[x, pl.ds(0, g.layers), pl.ds(0, lw)] = bq_in[...]

    pad = g.rows - g.flat_rows
    if pad:
        buf[x, pl.ds(g.flat_rows, pad), :] = jnp.zeros((pad, LANES), BF16)

    Q = CH // 4
    g0 = 2 * py + pz
    gy = 2 * (1 - py) + pz
    gz = 2 * py + 1 - pz
    gd = 2 * (1 - py) + 1 - pz

    def push(blk, k, part, dev, r_sem):
        r = buf.at[blk, pl.ds(pl.multiple_of(k * CH + part * Q, 8), Q)]
        remote(r, r, send, r_sem, dev).start()

    def await_quarters(n, sem):
        wait_like(buf.at[0, pl.ds(0, n * Q)], sem)

    def first(k):
        push(x, k, g0, dev_p, ra.at[k])
        push(x, k, g0, dev_m, ra.at[k])

    def stage1(k):
        await_quarters(2, ra.at[k])
        for blk in (xm, xp):
            push(blk, k, g0, dev_y, rb.at[k])
            push(blk, k, g0, dev_z, rb.at[k])

    def stage2(k):
        await_quarters(4, rb.at[k])
        push(xm, k, gz, dev_y, rc.at[k])
        push(xp, k, gy, dev_z, rc.at[k])

    def stage3(k):
        await_quarters(2, rc.at[k])
        for part in (g0, gy):
            push(xm, k, part, dev_p, rd.at[k])
        for part in (gz, gd):
            push(xp, k, part, dev_m, rd.at[k])

    def stage4(k):
        await_quarters(4, rd.at[k])

    K = g.chunks

    def tick(t):
        split = need(g.lr, 0)
        for lag, stage, lo, hi in ((EARLY_LAG, stage3, 0, split), (LAGS[2], stage3, split, K), (LAGS[0], stage1, 0, K), (LAGS[1], stage2, 0, K)):
            @pl.when((t - lag >= lo) & (t - lag < hi))
            def _(lag=lag, stage=stage):
                stage(t - lag)

        @pl.when(t + LA < K)
        def _():
            first(t + LA)

    def need(rows_end, lag):
        return -(-(rows_end - g.o0) // CH) + lag

    lane = lax.broadcasted_iota(jnp.int32, (1, LANES), 1)
    scale2 = LOG2E / math.sqrt(hd)

    def modulated(l, j, cond_ln, act_of):
        c_in = (cond_ln * ascale_in[l, pl.ds(j, 1), :]).astype(BF16)
        gain = jax.nn.sigmoid(dot_nn(c_in, adabuf[l * 2 + j, 0]) + abias_in[l, pl.ds(j, 1), :])
        shift = dot_nn(c_in, adabuf[l * 2 + j, 1])
        return (gain * normed(act_of().astype(F32)) + shift).astype(BF16)

    def row_blocks(body):
        for r in range(T // RB):
            body(pl.ds(r * RB, RB))

    full = pl.ds(0, T)

    def ada_rows(l, j, i, rows, n=0):
        xbuf[i, rows, :] = modulated(l, j, lnbuf[i, rows, :], lambda: abuf[i, rows, :])
        remote(xbuf.at[i, rows], xbuf.at[own + i, rows], sx.at[i, n], rx.at[i, n], dev_c).start()

    def resid_rows(l, j, i, part_of, rows, n=0):
        ours = part_of(l, i, rows)
        gate = jax.nn.sigmoid(dot_nn(cbuf[i, rows, :], zerobuf[l * 2 + j]) + zbias_in[l, pl.ds(j, 1), :])
        wait_like(pbuf.at[i, rows], rp.at[i, n])
        act = (abuf[i, rows, :].astype(F32) + gate * (ours + pbuf[i, rows, :].astype(F32)).astype(BF16).astype(F32)).astype(BF16)
        abuf[i, rows, :] = act
        if j == 1:
            out[mine + i, rows, :] = act

    def part_rows(l, i, part_of, rows, n=0):
        sbuf[i, rows, :] = part_of(l, own + i, rows).astype(BF16)
        remote(sbuf.at[i, rows], pbuf.at[i, rows], sp.at[i, n], rp.at[i, n], dev_c).start()

    stage0 = 2 * own * nx

    def relay_box(v):
        return xbuf.at[v, pl.ds(0, lw), pl.ds(0, T)]

    def flat(s, l, off, n):
        return buf[s, pl.ds(pl.multiple_of(l * g.lr - g.o0 + off, 8), n), :]

    def bias_prep(rows_of):
        for h in range(g.heads):
            for j in range(g.tcol):
                col = pl.ds(j * LANES, LANES)
                bmbuf[h, :, col] = rows_of(g.b0 + (h * g.tcol + j) * T, T).astype(F32) * LOG2E + mcol[...]

    def project_dot(x_rows, rows_of):
        w = jnp.concatenate([rows_of(g.q0 + j * 4 * lw, 4 * lw) for j in range(g.ncol)], axis=1)
        return dot_nt(w, x_rows)

    def project_end(slot, proj, q_bias):
        qs, ks, vs, gs = slot
        qs[...] = (proj[:lw] + q_bias).astype(BF16)
        ks[...] = proj[lw:2 * lw].astype(BF16).T
        vs[...] = proj[2 * lw:3 * lw].astype(BF16)
        gs[...] = jax.nn.sigmoid(proj[3 * lw:])

    def scores(slot, h):
        qs, ks, _, _ = slot
        none = jnp.zeros((hd, T), BF16)
        q = jnp.concatenate([qs[pl.ds(h * hd, hd), :] if v == h else none for v in range(g.heads)], axis=0)
        return dot_nn(ks[...], q)

    def weights(h, s):
        z = s * scale2 + bmbuf[h]
        return jnp.exp2(z - jnp.max(z, axis=0, keepdims=True)).astype(BF16)

    def mix(slot, h, e, o_ref):
        _, _, vs, gs = slot
        mine_h = pl.ds(h * hd, hd)
        o = dot_nn(jnp.concatenate([vs[mine_h, :], jnp.ones((16, T), BF16)], axis=0), e)
        o_ref[mine_h, :] = (o[:hd] * (1.0 / o[hd:hd + 1]) * gs[mine_h, :]).astype(BF16)

    def project(slot, x_rows, rows_of, q_bias):
        project_end(slot, project_dot(x_rows, rows_of), q_bias)

    def pair(slot, o_ref, after, x_rows, rows_of, q_bias):
        s0 = scores(slot, 0)
        s1 = scores(slot, 1)
        proj = project_dot(x_rows, rows_of)
        e0 = weights(0, s0)
        mix(slot, 0, e0, o_ref)
        e1 = weights(1, s1)
        mix(slot, 1, e1, o_ref)
        project_end(after, proj, q_bias)
    slot_a = (qa, ka, va, ga)
    slot_b = (qb, kb, vb, gb)

    def ada_first(n, ready=lambda: None):
        slot = lax.rem(n, RING)
        s = sample_of(n, c)
        wait_like(hbuf.at[slot], s_in.at[0, slot])
        wait_like(cring.at[slot], s_in.at[1, slot])
        def rows_body(rows):
            out[s, rows, :] = modulated(0, 0, normed(cring[slot, rows, :].astype(F32)), lambda: hbuf[slot, rows, :])
        row_blocks(rows_body)
        ready()
        remote(out.at[s], out.at[s], sx0, rx0.at[n], dev_c).start()
        @pl.when(n + RING < steps)
        def _():
            load_sample(n + RING)

    def qb_rows(off, n):
        return qb0[pl.ds(off, n), :]

    ada_cps[0].wait()
    load_attn(0, lambda off, n: qb0.at[pl.ds(off, n)], s_loc.at[0])
    for n in range(1, RING):
        load_sample(n)
    load_attn(1, own_rows(1), s_loc.at[2])
    load_rest(1, own_rows(1), s_loc.at[2])
    for cp in (cond_cp, zero_cps[0], *ada_cps[1:], *zero_cps[1:]):
        cp.start()
    early = (g.lr - g.o0) // CH

    def open_links():
        pl.semaphore_wait(barrier, len(devs))
        wait_like(buf.at[x, pl.ds(0, g.lr - g.o0)], s_loc.at[1])
        for k in range(min(LA, early)):
            first(k)
    ada_first(0, open_links)
    mask_col = jnp.broadcast_to((mask_in[...].astype(F32) - 1.0) * (1e9 * LOG2E), (8, T)).T
    mcol[...] = jnp.broadcast_to(mask_col[:, 0:1], (T, LANES))

    def put_first(off, v):
        qb0[pl.ds(off, T), :] = v
    turn_bias(0, put_first)
    load_bias(1)
    wait_like(qb0.at[pl.ds(0, g.b0)], s_loc.at[0])
    bias_prep(qb_rows)
    for d in (dev_p, dev_m, dev_o):
        remote(bqbuf.at[x], bqbuf.at[x], s_bq, r_bq, d).start()
    q_bias0 = bqbuf[x].T[:lw, 0:1]
    project(slot_a, out[sample_of(0, c)], qb_rows, q_bias0)
    wait_like(buf.at[x, pl.ds(0, g.lr - g.o0 + g.b0)], s_loc.at[2])
    for k in range(min(LA, early), LA):
        first(k)

    def put_second(off, v):
        buf[x, pl.ds(g.lr - g.o0 + off, T), :] = v

    def first_steps(m, carry):
        @pl.when(m == 1)
        def _():
            turn_bias(1, put_second)
            act_cp.start()

        @pl.when(m + 1 < steps)
        def _():
            ada_first(m + 1)

        def slot_of(pair, core):
            return jnp.where(pair == c, 0, own) + core

        def place_of(u, core):
            slot = slot_of(pair_of(m), core) * nx + x
            return slot, jnp.where(m < steps - own, stage0 + CORES * m + u, slot)

        def send(u, slot, place):
            @pl.when(m == 0)
            def _():
                remote(obuf.at[place], relay_box(u), s_o, r_rel.at[u], dev_p).start()

            @pl.when(m == 1)
            def _():
                remote(obuf.at[place], relay_box(CORES + u), s_o, r_rel.at[CORES + u], dev_m).start()

            @pl.when((m >= own) & (m < steps - own))
            def _():
                remote(obuf.at[place], obuf.at[slot], s_o, r_o, {'tp': chip_of(m) * CORES + c}).start()

        def forward(pair, dev, source):
            for u, core in enumerate((c, 1 - c)):
                r = relay_box(pair * CORES + u)
                wait_like(r, r_rel.at[pair * CORES + u])
                remote(r, obuf.at[slot_of(pair, core) * nx + source], s_o, r_o, dev).start()

        @pl.when(m == own + 1)
        def _():
            forward(0, dev_p, xm)

        @pl.when(m == own + 2)
        def _():
            forward(1, dev_m, xp)
        wait_like(out.at[0], rx0.at[m])
        slot, place = place_of(0, c)
        pair(slot_a, obuf.at[place], slot_b, out[sample_of(m, 1 - c)], qb_rows, q_bias0)
        send(0, slot, place)
        slot, place = place_of(1, 1 - c)
        pair(slot_b, obuf.at[place], slot_a, out[sample_of(jnp.minimum(m + 1, steps - 1), c)], qb_rows, q_bias0)
        send(1, slot, place)

        @pl.when(m >= HELD)
        def _():
            tick(m - HELD)
        return carry
    lax.fori_loop(0, steps, first_steps, 0)

    cond_cp.wait()
    act_cp.wait()
    for i in range(own):
        lnbuf[i] = normed(cbuf[i].astype(F32))
    for cp in (*ada_cps[1:], *zero_cps):
        cp.wait()
    remote_pieces = CORES * (steps - own)
    wait_like(obuf.at[pl.ds(stage0, remote_pieces)], r_o)
    wait_like(obuf.at[pl.ds(0, remote_pieces + CORES * own)], s_o)
    wait_like(out.at[pl.ds(0, steps)], sx0)

    def attn_part(l, i, rows):
        lhs = jnp.concatenate([obuf[i * nx + s, :, rows] for s in range(nx)], axis=0)
        rhs = jnp.concatenate([jnp.concatenate([flat(s, l, g.o0 + j * lw, lw) for s in range(nx)], axis=0) for j in range(g.ncol)], axis=1)
        return lax.dot_general(lhs, rhs, (((0,), (0,)), ((), ())), preferred_element_type=F32)

    def up_rows(l, i, rows=full):
        y = xbuf[i, rows, :]
        pre = []
        for p in range(nx // 2):
            w = jnp.concatenate([jnp.concatenate([flat(2 * p + e, l, g.u0 + j * 2 * hu, 2 * hu) for j in range(g.ncol)], axis=1) for e in range(2)], axis=0)
            pre.append(dot_nt(y, w))
        for p in range(nx // 2):
            mids = []
            for e in range(2):
                ua, ub, uc = (pre[p][:, (3 * e + v) * LANES:(3 * e + v + 1) * LANES] for v in range(3))
                side = (3 * p + 2 * e) * LANES
                hbuf[i, rows, side:side + LANES] = (jax.nn.silu(ua) * uc).astype(BF16)
                act = jax.nn.silu(ub)
                mids.append(act * pltpu.roll(ub, half, 1) if e == 0 else pltpu.roll(act, half, 1) * ub)
            mid = (3 * p + 1) * LANES
            hbuf[i, rows, mid:mid + LANES] = jnp.where(lane < half, mids[0], mids[1]).astype(BF16)

    def trans_part(l, i, rows):
        cols = []
        for j in range(g.ncol):
            v = []
            for p in range(nx // 2):
                v.append(flat(2 * p, l, g.d0 + j * hu, hu))
                v.append(flat(2 * p + 1, l, g.d0 + j * hu + LANES, half))
                v.append(flat(2 * p + 1, l, g.d0 + j * hu, LANES))
            cols.append(jnp.concatenate(v, axis=0))
        return dot_nn(hbuf[i, rows, :], jnp.concatenate(cols, axis=1))

    PR = OUT_ROWS
    npc = T // PR
    tpp, tpm, tpo = (v * CORES + c for v in (xp, xm, xo))

    def orow(blk, p, lo=0, n=PR):
        return out.at[blk * own + p // npc, pl.ds(pl.multiple_of(lax.rem(p, npc) * PR, PR) + lo, n)]

    def opush(r, dev, sem):
        remote(r, r, osend, sem, dev).start()

    def oawait(halves, sem):
        wait_like(out.at[0, pl.ds(0, halves * PR // 2)], sem)

    def out_first(p):
        opush(orow(tp, p), dev_p, o_a.at[p])
        opush(orow(tp, p), dev_m, o_a.at[p])
        opush(orow(tp, p), dev_c, o_p0.at[p])

    def out_relay(p):
        oawait(4, o_a.at[p])
        opush(orow(tpm, p, 0, PR // 2), dev_p, o_d.at[p])
        opush(orow(tpp, p, PR // 2, PR // 2), dev_m, o_d.at[p])
        opush(orow(tpm, p), dev_c, o_p1.at[p])
        opush(orow(tpp, p), dev_c, o_p1.at[p])

    t0 = steps - HELD
    t1 = t0 + TAIL_TICKS
    assert K + LAGS[-1] <= t1 + nx and need(g.d0, LAGS[-1]) <= t0 + 2 and need(g.lr, LAGS[-1]) <= t0 + 4
    assert need(g.lr + g.o0, LAGS[-1]) <= t1 + nx - 1 and need(g.lr + g.o0, LAGS[2]) <= t1

    def arrived(lo, hi):
        for k in range(lo, hi):
            stage4(k)

    k_o, k_u, k_d = (need(v, 0) for v in (g.u0, g.d0, g.lr))
    def each(count):
        def run(body):
            def step(i, carry):
                body(i)
                return carry
            lax.fori_loop(0, count, step, 0)
        return run

    arrived(0, k_o)

    @each(own)
    def _(i):
        part_rows(0, i, attn_part, full)

    @each(own)
    def _(i):
        resid_rows(0, 0, i, attn_part, full)
        ada_rows(0, 1, i, full)
        tick(t0 + i)
    arrived(k_o, k_u)

    @each(2 * own)
    def _(i):
        @pl.when(i >= own)
        def _():
            wait_like(xbuf.at[0], rx.at[i - own, 0])
        up_rows(0, i)

        @pl.when(lax.rem(i, 2) == 1)
        def _():
            tick(t0 + 2 + i // 2)
    arrived(k_u, k_d)

    @each(own)
    def _(i):
        wait_like(sbuf.at[0], sp.at[i, 0])
        part_rows(0, i, trans_part, full)
        wait_like(xbuf.at[0], sx.at[i, 0])

    @each(own)
    def _(i):
        resid_rows(0, 1, i, trans_part, full)
        ada_rows(1, 0, i, full)

        @pl.when(i < TAIL_TICKS - 4)
        def _():
            tick(t0 + 4 + i)
    wait_like(bqbuf.at[pl.ds(0, nx - 1)], r_bq)

    k_q, k_o, k_u, k_d = (need(g.lr + v, 0) for v in (g.o0, g.u0, g.d0, g.lr))
    first_k = need(g.lr, 0)

    def shard_of(q):
        return lax.rem(x + jnp.where(q == 0, 0, jnp.where(q == 1, nx - 1, q - 1)), nx)

    def rows_from(s):
        return lambda off, n: flat(s, 1, off, n)

    def q_bias1(s):
        return bqbuf[s].T[:lw, 1:2]

    def half_layer(hf, carry):
        def once(body):
            pl.when(hf == 0)(body)

        project(slot_a, xbuf[hf], rows_from(x), q_bias1(x))
        wait_like(xbuf.at[own + hf], rx.at[hf, 0])

        def shard(q, inner):
            s = shard_of(q)
            after = shard_of(jnp.minimum(q + 1, nx - 1))
            bias_prep(rows_from(s))
            pl.when((hf > 0) & (q == nx - 1))(lambda: out_relay(0))
            pair(slot_a, obuf.at[hf * nx + s], slot_b, xbuf[own + hf], rows_from(s), q_bias1(s))

            @pl.when(hf == 0)
            def _():
                tick(t1 + q)

                @pl.when(q == nx - 2)
                def _():
                    arrived(first_k, k_q)
            pair(slot_b, obuf.at[(own + hf) * nx + s], slot_a, xbuf[hf], rows_from(after), q_bias1(after))
            return inner
        lax.fori_loop(0, nx, shard, 0)
        once(lambda: arrived(k_q, k_o))
        ha, hb = (pl.ds(v * PR, PR) for v in range(2))
        wait_like(sbuf.at[hf], sp.at[hf, 0])
        wait_like(xbuf.at[hf], sx.at[hf, 0])
        part_rows(1, hf, attn_part, ha, 0)
        part_rows(1, hf, attn_part, hb, 1)
        resid_rows(1, 0, hf, attn_part, ha, 0)
        ada_rows(1, 1, hf, ha, 0)
        once(lambda: arrived(k_o, k_u))
        up_rows(1, hf, ha)
        resid_rows(1, 0, hf, attn_part, hb, 1)
        ada_rows(1, 1, hf, hb, 1)
        pl.when(hf > 0)(lambda: out_relay(1))
        wait_like(xbuf.at[own + hf, ha], rx.at[hf, 0])
        up_rows(1, own + hf, ha)
        once(lambda: arrived(k_u, k_d))
        wait_like(sbuf.at[hf, ha], sp.at[hf, 0])
        part_rows(1, hf, trans_part, ha, 0)
        up_rows(1, hf, hb)
        resid_rows(1, 1, hf, trans_part, ha, 0)
        out_first(hf * npc)
        wait_like(xbuf.at[own + hf, hb], rx.at[hf, 1])
        up_rows(1, own + hf, hb)
        wait_like(sbuf.at[hf, hb], sp.at[hf, 1])
        part_rows(1, hf, trans_part, hb, 1)
        resid_rows(1, 1, hf, trans_part, hb, 1)
        out_first(hf * npc + 1)
        for n, rows in enumerate((ha, hb)):
            wait_like(xbuf.at[hf, rows], sx.at[hf, n])
            wait_like(sbuf.at[hf, rows], sp.at[hf, n])
        return carry

    lax.fori_loop(0, own, half_layer, 0)
    for p in range(npc, own * npc):
        out_relay(p)
    for p in range(own * npc):
        oawait(2, o_d.at[p])
        opush(orow(tpo, p), dev_c, o_p2.at[p])
    for p in range(own * npc):
        oawait(2, o_p0.at[p])
        oawait(4, o_p1.at[p])
        oawait(2, o_p2.at[p])
    wait_like(out.at[pl.ds(0, 7 * own)], osend)
    wait_like(buf.at[pl.ds(0, 3)], send)
    wait_like(bqbuf.at[pl.ds(0, nx - 1)], s_bq)


def finish(src, dst, sem):
    cps = [pltpu.make_async_copy(src.at[v], dst.at[v], sem.at[v]) for v in range(src.shape[0])]
    for cp in cps:
        cp.start()
    for cp in cps:
        cp.wait()


def solution(mesh):
    def body(token_act, token_cond, pair_bias, token_mask, ada_scale, ada_w, ada_bias, zero_w, zero_b, w_qkvg, b_q, w_o, w_up, w_down):
        g = Geometry(mesh, token_act.shape, token_cond.shape, pair_bias.shape, w_qkvg.shape, w_up.shape)
        L, D, C, T, own, nx = g.layers, g.width, g.cond_dim, g.tokens, g.own, g.nx
        ada = ada_w.transpose(0, 1, 3, 2, 4).reshape(2 * L, 2, C, D)
        zero = zero_w.transpose(0, 2, 1, 3).reshape(2 * L, C, D)
        vm = pl.BlockSpec(memory_space=pltpu.VMEM)
        hbm = pl.BlockSpec(memory_space=pl.ANY)
        dma = pltpu.SemaphoreType.DMA
        npc = own * (T // OUT_ROWS)
        K = g.chunks
        steps = nx * own
        gathered = pl.pallas_call(
            functools.partial(kernel, g),
            out_shape=pltpu.VMEM(token_act.shape, BF16),
            in_specs=[hbm, hbm, hbm, vm, vm, hbm, vm, hbm, vm, hbm, vm, hbm, hbm, hbm],
            out_specs=vm,
            scratch_shapes=[
                pltpu.VMEM((nx, g.rows, LANES), BF16),
                pltpu.VMEM((g.o0, LANES), BF16),
                pltpu.VMEM((2 * own, T, D), BF16),
                pltpu.VMEM((own, T, D), BF16),
                pltpu.VMEM((own, T, D), BF16),
                pltpu.VMEM((own, T, D), BF16),
                pltpu.VMEM((2 * own * nx + CORES * (steps - own), g.lw, T), BF16),
                pltpu.VMEM((2 * own, T, nx * g.hu), BF16),
                pltpu.VMEM((RING, T, C), BF16),
                pltpu.VMEM((own, T, C), BF16),
                pltpu.VMEM((own, T, C), F32),
                pltpu.VMEM((2 * L, 2, C, D), BF16),
                pltpu.VMEM((2 * L, C, D), BF16),
                pltpu.VMEM((nx, 8, LANES), F32),
                pltpu.VMEM((T, LANES), F32),
                pltpu.VMEM((g.heads, T, T), F32),
                pltpu.VMEM((g.lw, T), BF16),
                pltpu.VMEM((T, g.lw), BF16),
                pltpu.VMEM((g.lw, T), BF16),
                pltpu.VMEM((g.lw, T), F32),
                pltpu.VMEM((g.lw, T), BF16),
                pltpu.VMEM((T, g.lw), BF16),
                pltpu.VMEM((g.lw, T), BF16),
                pltpu.VMEM((g.lw, T), F32),
                dma((3,)), dma((3,)), dma, dma((4 * L,)), dma((2, RING)), dma,
                dma((K,)), dma((K,)), dma((K,)), dma((K,)),
                dma, dma, dma, dma((steps,)), dma, dma, dma((CORES * own,)),
                dma((own, 2)), dma((own, 2)), dma((own, 2)), dma((own, 2)),
                dma, dma((npc,)), dma((npc,)), dma((npc,)), dma((npc,)), dma((npc,)),
            ],
            compiler_params=pltpu.CompilerParams(collective_id=0, has_side_effects=True, vmem_limit_bytes=207 << 18),
            name='blocks',
        )(token_act, token_cond, pair_bias, token_mask.reshape(1, T), ada_scale, ada, ada_bias, zero, zero_b, w_qkvg.transpose(0, 2, 3, 1), b_q, w_o, w_up.transpose(0, 2, 3, 1), w_down)
        gathered = pltpu.with_memory_space_constraint(gathered, pltpu.VMEM)
        return pl.pallas_call(
            finish,
            out_shape=jax.ShapeDtypeStruct(token_act.shape, BF16),
            in_specs=[vm],
            out_specs=pl.BlockSpec(memory_space=pltpu.HBM),
            scratch_shapes=[dma((token_act.shape[0],))],
            compiler_params=pltpu.CompilerParams(vmem_limit_bytes=1 << 20),
            name='finish',
        )(gathered)

    everywhere = P()
    in_specs = (P('dp', None, None), P('dp', None, None), P(None, 'tp', None, None), P(None), everywhere, everywhere, everywhere, everywhere, everywhere, P(None, None, None, 'tp'), P(None, 'tp'), P(None, 'tp', None), P(None, None, None, 'tp'), P(None, 'tp', None))
    return jax.shard_map(body, mesh=mesh, in_specs=in_specs, out_specs=P('dp', None, None), check_vma=False)
```
